32 devices in a mesh: row: 8 (over z, x), col: 4 (over y, core).
Axes of the slice: x: 2, y: 2, z: 4, core: 2. Of those that a mesh axis runs over, the one named last changes fastest.
Arguments:
- snapshot: bfloat16 [512, 256, 512], P('row', 'col'), may hold values from -6 to 6
- basis_two: bfloat16 [256, 128], P('col'), may hold values from -0.375 to 0.375
- basis_three: bfloat16 [512, 128], replicated, may hold values from -0.25 to 0.25
Outputs:
- gram: float32 [512, 512], P('row', 'col')
The draws below stay inside these ranges and needn't reach their ends.
All inputs are finite; a program needn't handle non-finite values.
Results may differ from the reference program's by a relative error of at most 0.0017.
Values may be sent and summed in bfloat16 or wider, within the bound.
No kernel may reach another device: no remote copies, remote signals or barrier semaphores. Data moves between devices by JAX's collectives and lax.ppermute only.
A program may use at most 64 MiB of HBM per device.

```python
import jax
import jax.numpy as jnp
from jax import lax

I3 = 512
R2 = 128
R3 = 128
I1 = 512
I2 = 256


def levels(own_key, dims, cuts, smallest, top_value):
    level = 1.0
    for dim, blocks in cuts:
        steps = jax.random.uniform(jax.random.fold_in(jax.random.fold_in(own_key, 6), dim), (blocks,), jnp.float32, smallest / len(cuts), top_value / len(cuts))
        level = level * jnp.repeat(jnp.exp(steps), dims[dim] // blocks).reshape((-1,) + (1,) * (len(dims) - 1 - dim))
    return level


def normal_values(stream_key, dims, deviation, reach, split=(), held_as=jnp.bfloat16):
    result = jax.random.normal(stream_key, dims, jnp.float32) * deviation
    if len(split) > 0:
        result = levels(stream_key, dims, split, -0.22, 0.18) * result
    return jnp.clip(result, min=-reach, max=reach).astype(held_as)


def setup_inputs(seed: int = 0) -> dict:
    seeds = jax.random.split(jax.random.key(seed), 4)
    snapshot = normal_values(seeds[0], (I1, I2, I3), 1.0, 6.0, ((0, 8), (1, 4)))
    basis_two = normal_values(seeds[1], (I2, R2), I2 ** -0.5, 0.375, ((0, 4),))
    basis_three = normal_values(seeds[2], (I3, R3), I3 ** -0.5, 0.25)
    return dict(snapshot=snapshot, basis_two=basis_two, basis_three=basis_three)


def reference(snapshot, basis_two, basis_three):
    block_rows = 8 if I1 % 8 == 0 else 1
    blocks = snapshot.reshape(I1 // block_rows, block_rows, I2, I3)
    second = basis_two.astype(jnp.float32)

    def project(block):
        inner = jnp.dot(block.reshape(block_rows * I2, I3), basis_three, preferred_element_type=jnp.float32)
        inner = lax.optimization_barrier(inner.astype(jnp.bfloat16)).astype(jnp.float32)
        inner = inner.reshape(block_rows, I2, R3)
        return jnp.einsum("abr,bq->aqr", inner, second, precision=lax.Precision.HIGHEST)

    projected = lax.map(project, blocks).reshape(I1, R2 * R3)
    rounded = projected.astype(jnp.bfloat16)
    total = jnp.dot(rounded, rounded.T, preferred_element_type=jnp.float32)
    return total * (1.0 / (R2 * R3))
```

```python
import functools

import jax
import jax.numpy as jnp
from jax import lax
from jax.experimental import pallas as pl
from jax.experimental.pallas import tpu as pltpu
from jax.sharding import PartitionSpec as P

VMEM = pltpu.VMEM
MIB = 1024 * 1024


def swap_blocks(tiles, width):
    count = len(tiles)
    lane = lax.broadcasted_iota(jnp.int32, tiles[0].shape, 1) // width
    outs = []
    for j in range(count):
        out = None
        for g in range(count):
            shift = ((g - j) * width) % (count * width)
            moved = tiles[g] if shift == 0 else pltpu.roll(tiles[g], shift, 1)
            out = moved if out is None else jnp.where(lane == g, moved, out)
        outs.append(out)
    return outs


def project_three_kernel(chunks, snap, three, two, out, buf, three_buf, two_buf, sems):
    groups, steps, cells_two, cells_three = snap.shape
    per = steps // chunks
    width = three.shape[1] // groups
    copies = [
        pltpu.make_async_copy(three, three_buf, sems.at[chunks]),
        pltpu.make_async_copy(two, two_buf, sems.at[chunks + 1]),
    ]
    for n in range(chunks):
        part = (slice(None), pl.ds(n * per, per))
        copies.append(pltpu.make_async_copy(snap.at[part], buf.at[part], sems.at[n]))
    for copy in copies:
        copy.start()
    copies[0].wait()
    weights = three_buf[...]
    for n in range(chunks):
        copies[2 + n].wait()
        rows = per * cells_two
        inner = [
            jnp.dot(
                buf[g, n * per : (n + 1) * per].reshape(rows, cells_three),
                weights,
                preferred_element_type=jnp.float32,
            )
            for g in range(groups)
        ]
        for j, piece in enumerate(swap_blocks(inner, width)):
            out[j, n * rows : (n + 1) * rows, :] = piece.astype(jnp.bfloat16)
    copies[1].wait()
    for j in range(groups):
        out[j, steps * cells_two :, :] = two_buf[...]


def project_three(snapshot, basis_two, basis_three, cols):
    cells_one, cells_two, cells_three = snapshot.shape
    ranks_two = basis_two.shape[1]
    ranks_three = basis_three.shape[1]
    steps = cells_one // cols
    snap = snapshot.reshape(cols, steps, cells_two, cells_three)
    if ranks_two != 128 or ranks_three != 128 or steps % 16 or ranks_three // cols < 32:
        inner = jnp.einsum(
            "gtbc,cr->gtbr", snap, basis_three, preferred_element_type=jnp.float32
        ).astype(jnp.bfloat16)
        inner = inner.reshape(cols, steps, cells_two, cols, ranks_three // cols)
        inner = inner.transpose(3, 1, 2, 0, 4)
        inner = inner.reshape(cols, steps * cells_two, ranks_three)
        two = jnp.broadcast_to(basis_two, (cols,) + basis_two.shape)
        return jnp.concatenate([inner, two], axis=1)
    chunks = 4
    rows = (steps + 1) * cells_two
    return pl.pallas_call(
        functools.partial(project_three_kernel, chunks),
        out_shape=jax.ShapeDtypeStruct((cols, rows, ranks_three), jnp.bfloat16),
        in_specs=[pl.BlockSpec(memory_space=pltpu.HBM)] * 3,
        out_specs=pl.BlockSpec(memory_space=VMEM),
        scratch_shapes=[
            VMEM(snap.shape, jnp.bfloat16),
            VMEM(basis_three.shape, jnp.bfloat16),
            VMEM(basis_two.shape, jnp.bfloat16),
            pltpu.SemaphoreType.DMA((chunks + 2,)),
        ],
        compiler_params=pltpu.CompilerParams(vmem_limit_bytes=20 * MIB),
        name="project_three",
    )(snap, basis_three, basis_two)


def project_two_kernel(recv, out, held):
    cols, rows, width = recv.shape
    dests, part, _ = out.shape
    ranks_two = held.shape[0] // (dests * part // recv.shape[2])
    ranks_two = recv.shape[2]
    steps = dests * part // ranks_two
    cells = rows // (steps + 1)
    factor = jnp.concatenate([recv[j, steps * cells :, :] for j in range(cols)], axis=0)
    factor = factor.astype(jnp.float32).T.astype(jnp.bfloat16)
    for t in range(steps):
        inner = jnp.concatenate(
            [recv[j, t * cells : (t + 1) * cells, :] for j in range(cols)], axis=0
        )
        held[pl.ds(t, ranks_two, stride=steps), :] = jnp.dot(
            factor, inner, preferred_element_type=jnp.float32
        )
    out[...] = held[...].astype(jnp.bfloat16).reshape(out.shape)


def project_two(recv, rows, cells_two):
    cols, height, width = recv.shape
    steps = height // cells_two - 1
    ranks_two = width
    shape = (rows, steps * ranks_two // rows, width)
    if steps % 16 or width != 128 or ranks_two % rows:
        inner = recv[:, : steps * cells_two].reshape(cols, steps, cells_two, width)
        factor = recv[:, steps * cells_two :]
        full = jnp.einsum("jtbl,jbq->qtl", inner, factor, preferred_element_type=jnp.float32)
        return full.astype(jnp.bfloat16).reshape(shape)
    return pl.pallas_call(
        project_two_kernel,
        out_shape=jax.ShapeDtypeStruct(shape, jnp.bfloat16),
        in_specs=[pl.BlockSpec(memory_space=VMEM)],
        out_specs=pl.BlockSpec(memory_space=VMEM),
        scratch_shapes=[VMEM((steps * ranks_two, width), jnp.float32)],
        compiler_params=pltpu.CompilerParams(vmem_limit_bytes=20 * MIB),
        name="project_two",
    )(recv)


def gram_kernel(cols, recv, out, held):
    rows, part, width = recv.shape
    dests, cells_one, cells_out = out.shape
    steps = cells_one // cols
    ranks = part // steps
    block = width // cols
    for i in range(rows):
        for u in range(ranks // cols):
            tiles = [
                recv[i, (u * cols + p) * steps : (u * cols + p + 1) * steps, :].astype(
                    jnp.float32
                )
                for p in range(cols)
            ]
            for g, tile in enumerate(swap_blocks(tiles, block)):
                base = i * cells_one + g * steps
                held[base : base + steps, u * width : (u + 1) * width] = tile.astype(
                    jnp.bfloat16
                )
    right = held[...]
    for i in range(rows):
        left = held[i * cells_one : (i + 1) * cells_one, :]
        gram = lax.dot_general(
            left, right, (((1,), (1,)), ((), ())), preferred_element_type=jnp.float32
        ).astype(out.dtype)
        for j in range(cols):
            out[i * cols + j] = gram[:, j * cells_out : (j + 1) * cells_out]


def partial_gram(recv, cells_one, cols):
    rows, part, width = recv.shape
    steps = cells_one // cols
    ranks = part // steps
    block = width // cols
    cells_out = rows * cells_one // cols
    shape = (rows * cols, cells_one, cells_out)
    if steps % 16 or width != 128 or ranks % cols or cells_out % 128:
        flat = recv.reshape(rows, ranks, steps, cols, block).transpose(0, 3, 2, 1, 4)
        flat = flat.reshape(rows * cells_one, ranks * block)
        gram = jnp.einsum("ak,ek->ae", flat, flat, preferred_element_type=jnp.float32)
        gram = gram.reshape(rows, cells_one, cols, cells_out).transpose(0, 2, 1, 3)
        return gram.reshape(shape).astype(jnp.bfloat16)
    return pl.pallas_call(
        functools.partial(gram_kernel, cols),
        out_shape=jax.ShapeDtypeStruct(shape, jnp.bfloat16),
        in_specs=[pl.BlockSpec(memory_space=VMEM)],
        out_specs=pl.BlockSpec(memory_space=VMEM),
        scratch_shapes=[VMEM((rows * cells_one, ranks * block), jnp.bfloat16)],
        compiler_params=pltpu.CompilerParams(vmem_limit_bytes=20 * MIB),
        name="partial_gram",
    )(recv)


def on_device(rows, cols, snapshot, basis_two, basis_three):
    cells_one, cells_two, _ = snapshot.shape
    ranks_two = basis_two.shape[1]
    ranks_three = basis_three.shape[1]
    pieces = project_three(snapshot, basis_two, basis_three, cols)
    pieces = lax.all_to_all(pieces, "col", split_axis=0, concat_axis=0, tiled=True)
    shares = project_two(pieces, rows, cells_two)
    shares = lax.all_to_all(shares, "row", split_axis=0, concat_axis=0, tiled=True)
    parts = partial_gram(shares, cells_one, cols)
    parts = lax.all_to_all(parts, ("row", "col"), split_axis=0, concat_axis=0, tiled=True)
    total = jnp.sum(parts.astype(jnp.float32), axis=0)
    return total * (1.0 / (ranks_two * ranks_three))


def solution(mesh):
    in_specs = (P("row", "col", None), P("col", None), P())
    return jax.shard_map(
        functools.partial(on_device, mesh.shape["row"], mesh.shape["col"]),
        mesh=mesh,
        in_specs=in_specs,
        out_specs=P("row", "col"),
        check_vma=False,
    )
```

```python
import functools

import jax
import jax.numpy as jnp
from jax import lax
from jax.experimental import pallas as pl
from jax.experimental.pallas import tpu as pltpu
from jax.sharding import Mesh
from jax.sharding import PartitionSpec as P

VMEM = pltpu.VMEM
MIB = 1024 * 1024
PLANE = ("x", "y", "core")


def in_vmem(count):
    return [pl.BlockSpec(memory_space=VMEM)] * count


def slots(count):
    return list(reversed(range(count)))


def place(axes):
    index = 0
    for axis in axes:
        index = index * lax.axis_size(axis) + lax.axis_index(axis)
    return index


def swap_blocks(tiles, width, me=None):
    tiles = list(tiles)
    lane = lax.broadcasted_iota(jnp.int32, tiles[0].shape, 1) // width
    lanes = len(tiles) * width
    step = 1
    while step < len(tiles):
        low = lax.bitwise_and(lane, step) == 0
        for i in range(len(tiles)):
            if i & step:
                continue
            one, two = tiles[i], tiles[i | step]
            zeros = jnp.where(low, one, pltpu.roll(two, step * width, 1))
            ones = jnp.where(low, pltpu.roll(one, lanes - step * width, 1), two)
            if me is None:
                tiles[i], tiles[i | step] = zeros, ones
            else:
                flip = lax.bitwise_and(me, step) != 0
                tiles[i] = jnp.where(flip, ones, zeros)
                tiles[i | step] = jnp.where(flip, zeros, ones)
        step *= 2
    return tiles


def project_three_kernel(parts, snap, three, two, *rest):
    groups, steps, cells_two, cells_three = snap.shape
    outs = rest[:groups]
    buf, three_buf, two_buf, sems = rest[groups:]
    per = steps // parts
    width = three.shape[1] // groups
    me = place(PLANE)
    copies = [
        pltpu.make_async_copy(three, three_buf, sems.at[parts]),
        pltpu.make_async_copy(two, two_buf, sems.at[parts + 1]),
    ]
    for n in range(parts):
        part = (slice(None), pl.ds(n * per, per))
        copies.append(pltpu.make_async_copy(snap.at[part], buf.at[part], sems.at[n]))
    for copy in copies:
        copy.start()
    copies[0].wait()
    weights = three_buf[...]
    for n in range(parts):
        copies[2 + n].wait()
        rows = per * cells_two
        inner = [
            jnp.dot(
                buf[g, n * per : (n + 1) * per].reshape(rows, cells_three),
                weights,
                preferred_element_type=jnp.float32,
            )
            for g in range(groups)
        ]
        pieces = swap_blocks(inner, width, me)
        for s, out in zip(slots(groups), outs):
            out[n * rows : (n + 1) * rows, :] = pieces[s].astype(jnp.bfloat16)
    copies[1].wait()
    for out in outs:
        if out.shape[0] > steps * cells_two:
            out[steps * cells_two :, :] = two_buf[...]


def project_three(snapshot, basis_two, basis_three, plane, cols, tiled):
    cells_one, cells_two, cells_three = snapshot.shape
    ranks_three = basis_three.shape[1]
    steps = cells_one // plane
    snap = snapshot.reshape(plane, steps, cells_two, cells_three)
    if not tiled:
        inner = jnp.einsum(
            "gtbc,cr->gtbr", snap, basis_three, preferred_element_type=jnp.float32
        ).astype(jnp.bfloat16)
        inner = inner.reshape(plane, steps, cells_two, plane, ranks_three // plane)
        inner = inner.transpose(3, 1, 2, 0, 4)
        inner = inner.reshape(plane, steps * cells_two, ranks_three)
        pieces = [jnp.take(inner, place(PLANE) ^ s, axis=0) for s in slots(plane)]
        return [
            jnp.concatenate([piece, basis_two]) if s < cols else piece
            for s, piece in zip(slots(plane), pieces)
        ]
    parts = 4
    outs = [
        jax.ShapeDtypeStruct(((steps + (s < cols)) * cells_two, ranks_three), jnp.bfloat16)
        for s in slots(plane)
    ]
    args = [
        pltpu.with_memory_space_constraint(arg, pltpu.HBM)
        for arg in (snap, basis_three, basis_two)
    ]
    return pl.pallas_call(
        functools.partial(project_three_kernel, parts),
        out_shape=outs,
        in_specs=[pl.BlockSpec(memory_space=pltpu.HBM)] * 3,
        out_specs=in_vmem(plane),
        scratch_shapes=[
            VMEM(snap.shape, jnp.bfloat16),
            VMEM(basis_three.shape, jnp.bfloat16),
            VMEM(basis_two.shape, jnp.bfloat16),
            pltpu.SemaphoreType.DMA((parts + 2,)),
        ],
        compiler_params=pltpu.CompilerParams(vmem_limit_bytes=20 * MIB),
        name="project_three",
    )(*args)


def project_two_kernel(plane, steps, *refs):
    recv, outs, held = refs[:plane], refs[plane:-1], refs[-1]
    cols = plane // 2
    part, ranks_two = outs[0].shape
    cells = recv[0].shape[0] // steps
    me = lax.axis_index("z")
    factor = jnp.concatenate([ref[steps * cells :, :] for ref in recv[cols:]], axis=0)
    factor = factor.astype(jnp.float32).T.astype(jnp.bfloat16)
    for side, refs in ((1, recv[:cols]), (0, recv[cols:])):
        for t in range(steps):
            inner = jnp.concatenate(
                [ref[t * cells : (t + 1) * cells, :] for ref in refs], axis=0
            )
            held[pl.ds(side * steps + t, ranks_two, stride=2 * steps), :] = jnp.dot(
                factor, inner, preferred_element_type=jnp.float32
            )
    for s, out in zip(slots(len(outs)), outs):
        base = pl.multiple_of(lax.bitwise_xor(me, s) * part, part)
        out[...] = held[pl.ds(base, part), :].astype(jnp.bfloat16)


def project_two(recv, steps, deep, tiled):
    plane = len(recv)
    cols = plane // 2
    height, width = recv[0].shape
    cells_two = height // steps
    part = 2 * steps * width // deep
    if not tiled:
        factor = jnp.stack([piece[height:] for piece in recv[cols:]])
        inner = jnp.stack([piece[:height] for piece in recv[cols:] + recv[:cols]])
        inner = inner.reshape(2, cols, steps, cells_two, width)
        full = jnp.einsum("xjtbl,jbq->qxtl", inner, factor, preferred_element_type=jnp.float32)
        full = full.astype(jnp.bfloat16).reshape(deep, part, width)
        return [jnp.take(full, lax.axis_index("z") ^ s, axis=0) for s in slots(deep)]
    return pl.pallas_call(
        functools.partial(project_two_kernel, plane, steps),
        out_shape=[jax.ShapeDtypeStruct((part, width), jnp.bfloat16)] * deep,
        in_specs=in_vmem(plane),
        out_specs=in_vmem(deep),
        scratch_shapes=[VMEM((2 * steps * width, width), jnp.float32)],
        compiler_params=pltpu.CompilerParams(vmem_limit_bytes=20 * MIB),
        name="project_two",
    )(*recv)


def gram_block(left, right):
    return lax.dot_general(
        left, right, (((1,), (1,)), ((), ())), preferred_element_type=jnp.float32
    )


def other_core_gram_kernel(plane, *refs):
    recv, (flat, out) = refs[:-2], refs[-2:]
    deep = len(recv)
    cells_one = flat.shape[0] // (2 * deep)
    halves, _, cells_out = out.shape
    part, width = recv[0].shape
    steps = cells_one // plane
    rows = 2 * steps
    block = width // plane
    me_z, me_x = lax.axis_index("z"), lax.axis_index("x")
    for s, ref in zip(slots(deep), recv):
        for u in range(part // rows // plane):
            tiles = [
                ref[q * rows : (q + 1) * rows, :].astype(jnp.float32)
                for q in range(u * plane, (u + 1) * plane)
            ]
            tiles = swap_blocks(tiles, block)
            for side in range(2):
                row = lax.bitwise_xor(me_z, s) * 2 + lax.bitwise_xor(me_x, side)
                base = pl.multiple_of(row * cells_one, cells_one)
                stacked = jnp.concatenate(
                    [tile[side * steps : (side + 1) * steps] for tile in tiles], axis=0
                )
                flat[pl.ds(base, cells_one), u * width : (u + 1) * width] = stacked.astype(
                    jnp.bfloat16
                )
    other = 1 - lax.axis_index("core")
    left = flat[...]
    for y in range(halves):
        base = pl.multiple_of((2 * y + other) * cells_out, cells_out)
        out[y] = gram_block(left, flat[pl.ds(base, cells_out), :])


def own_core_gram_kernel(scale, flat, recv, out):
    halves, _, cells_out = recv.shape
    cells_one = out.shape[1]
    core = lax.axis_index("core")
    left = flat[...]
    for y in range(halves):
        base = pl.multiple_of((2 * y + core) * cells_out, cells_out)
        gram = gram_block(left, flat[pl.ds(base, cells_out), :])
        gram = ((gram + recv[y]) * scale).astype(out.dtype)
        for i in range(out.shape[0] // halves):
            out[i * halves + y] = gram[i * cells_one : (i + 1) * cells_one, :]


def chip_gram(recv, cells_one, plane, scale, tiled):
    deep = len(recv)
    part, width = recv[0].shape
    steps = cells_one // plane
    ranks = part // (2 * steps)
    block = width // plane
    rows = 2 * deep
    cells = rows * cells_one
    halves = plane // 4
    cells_out = cells // (2 * halves)
    swap = [(0, 1), (1, 0)]
    if not tiled:
        flat = jnp.stack(recv[::-1]).reshape(deep, ranks, 2, steps, plane, block)
        flat = jnp.take(flat, lax.axis_index("z") ^ jnp.arange(deep), axis=0)
        flat = jnp.take(flat, lax.axis_index("x") ^ jnp.arange(2), axis=2)
        flat = flat.transpose(0, 2, 4, 3, 1, 5).reshape(cells, ranks * block)
        gram = gram_block(flat, flat).reshape(rows, cells_one, halves, 2, cells_out)
        gram = gram.transpose(3, 0, 2, 1, 4).reshape(2, rows * halves, cells_one, cells_out)
        core = lax.axis_index("core")
        sent = lax.ppermute(jnp.take(gram, 1 - core, axis=0), "core", swap)
        return ((jnp.take(gram, core, axis=0) + sent) * scale).astype(jnp.bfloat16)
    params = pltpu.CompilerParams(vmem_limit_bytes=20 * MIB)
    flat, other = pl.pallas_call(
        functools.partial(other_core_gram_kernel, plane),
        out_shape=[
            jax.ShapeDtypeStruct((cells, ranks * block), jnp.bfloat16),
            jax.ShapeDtypeStruct((halves, cells, cells_out), jnp.float32),
        ],
        in_specs=in_vmem(deep),
        out_specs=in_vmem(2),
        compiler_params=params,
        name="other_core_gram",
    )(*recv)
    other = lax.ppermute(other, "core", swap)
    return pl.pallas_call(
        functools.partial(own_core_gram_kernel, scale),
        out_shape=jax.ShapeDtypeStruct((rows * halves, cells_one, cells_out), jnp.bfloat16),
        in_specs=in_vmem(2),
        out_specs=in_vmem(1)[0],
        compiler_params=params,
        name="own_core_gram",
    )(flat, other)


def exchange(pieces, axis):
    count = len(pieces)
    assert count & (count - 1) == 0
    return [
        lax.ppermute(piece, axis, [(i, i ^ s) for i in range(count)]) if s else piece
        for s, piece in zip(slots(count), pieces)
    ]


def on_device(deep, cols, snapshot, basis_two, basis_three):
    cells_one = snapshot.shape[0]
    ranks_two, ranks_three = basis_two.shape[1], basis_three.shape[1]
    scale = 1.0 / (ranks_two * ranks_three)
    plane = 2 * cols
    steps = cells_one // plane
    tiled = (
        ranks_two == 128
        and ranks_three == 128
        and steps % 8 == 0
        and ranks_two // deep % plane == 0
        and 2 * deep * cells_one // cols % 128 == 0
    )
    pieces = project_three(snapshot, basis_two, basis_three, plane, cols, tiled)
    pieces = exchange(pieces, PLANE)
    shares = project_two(pieces, steps, deep, tiled)
    shares = exchange(shares, "z")
    parts = chip_gram(shares, cells_one, plane, scale, tiled)
    parts = lax.all_to_all(
        parts, ("z", "x", "y"), split_axis=0, concat_axis=0, tiled=True
    )
    return jnp.sum(parts.astype(jnp.float32), axis=0)


def solution(mesh):
    rows, cols = mesh.shape["row"], mesh.shape["col"]
    devices = mesh.devices.reshape(rows // 2, 2, cols // 2, 2)
    row, col = ("z", "x"), ("y", "core")
    return jax.shard_map(
        functools.partial(on_device, rows // 2, cols),
        mesh=Mesh(devices, row + col),
        in_specs=(P(row, col, None), P(col, None), P()),
        out_specs=P(row, col),
        check_vma=False,
    )
```

```python
import functools

import jax
import jax.numpy as jnp
from jax import lax
from jax.experimental import pallas as pl
from jax.experimental.pallas import tpu as pltpu
from jax.sharding import Mesh
from jax.sharding import PartitionSpec as P

VMEM = pltpu.VMEM
MIB = 1024 * 1024
PLANE = ("x", "y", "core")


def in_vmem(count):
    return [pl.BlockSpec(memory_space=VMEM)] * count


def slots(count):
    return list(reversed(range(count)))


def plane_slots(plane):
    cols = plane // 2
    return slots(cols) + [s ^ (cols // 2) for s in slots(plane)[:cols]]


def place(axes):
    index = 0
    for axis in axes:
        index = index * lax.axis_size(axis) + lax.axis_index(axis)
    return index


def swap_blocks(tiles, width, me=None):
    tiles = list(tiles)
    lane = lax.broadcasted_iota(jnp.int32, tiles[0].shape, 1) // width
    lanes = len(tiles) * width
    step = 1
    while step < len(tiles):
        low = lax.bitwise_and(lane, step) == 0
        for i in range(len(tiles)):
            if i & step:
                continue
            one, two = tiles[i], tiles[i | step]
            zeros = jnp.where(low, one, pltpu.roll(two, step * width, 1))
            ones = jnp.where(low, pltpu.roll(one, lanes - step * width, 1), two)
            if me is None:
                tiles[i], tiles[i | step] = zeros, ones
            else:
                flip = lax.bitwise_and(me, step) != 0
                tiles[i] = jnp.where(flip, ones, zeros)
                tiles[i | step] = jnp.where(flip, zeros, ones)
        step *= 2
    return tiles


def project_three_kernel(parts, snap, three, two, *rest):
    groups, steps, cells_two, cells_three = snap.shape
    outs = rest[:groups]
    buf, three_buf, two_buf, sems = rest[groups:]
    per = steps // parts
    width = three.shape[1] // groups
    me = place(PLANE)
    copies = [
        pltpu.make_async_copy(three, three_buf, sems.at[parts]),
        pltpu.make_async_copy(two, two_buf, sems.at[parts + 1]),
    ]
    for n in range(parts):
        part = (slice(None), pl.ds(n * per, per))
        copies.append(pltpu.make_async_copy(snap.at[part], buf.at[part], sems.at[n]))
    for copy in copies:
        copy.start()
    copies[0].wait()
    weights = three_buf[...]
    for n in range(parts):
        copies[2 + n].wait()
        rows = per * cells_two
        inner = [
            jnp.dot(
                buf[g, n * per : (n + 1) * per].reshape(rows, cells_three),
                weights,
                preferred_element_type=jnp.float32,
            )
            for g in range(groups)
        ]
        pieces = swap_blocks(inner, width, me)
        for s, out in zip(plane_slots(groups), outs):
            out[n * rows : (n + 1) * rows, :] = pieces[s].astype(jnp.bfloat16)
    copies[1].wait()
    for out in outs:
        if out.shape[0] > steps * cells_two:
            out[steps * cells_two :, :] = two_buf[...]


def project_three(snapshot, basis_two, basis_three, plane, cols, tiled):
    cells_one, cells_two, cells_three = snapshot.shape
    ranks_three = basis_three.shape[1]
    steps = cells_one // plane
    snap = snapshot.reshape(plane, steps, cells_two, cells_three)
    if not tiled:
        inner = jnp.einsum(
            "gtbc,cr->gtbr", snap, basis_three, preferred_element_type=jnp.float32
        ).astype(jnp.bfloat16)
        inner = inner.reshape(plane, steps, cells_two, plane, ranks_three // plane)
        inner = inner.transpose(3, 1, 2, 0, 4)
        inner = inner.reshape(plane, steps * cells_two, ranks_three)
        pieces = [jnp.take(inner, place(PLANE) ^ s, axis=0) for s in plane_slots(plane)]
        return [
            jnp.concatenate([piece, basis_two]) if s < cols else piece
            for s, piece in zip(plane_slots(plane), pieces)
        ]
    parts = 4
    outs = [
        jax.ShapeDtypeStruct(((steps + (s < cols)) * cells_two, ranks_three), jnp.bfloat16)
        for s in plane_slots(plane)
    ]
    args = [
        pltpu.with_memory_space_constraint(arg, pltpu.HBM)
        for arg in (snap, basis_three, basis_two)
    ]
    return pl.pallas_call(
        functools.partial(project_three_kernel, parts),
        out_shape=outs,
        in_specs=[pl.BlockSpec(memory_space=pltpu.HBM)] * 3,
        out_specs=in_vmem(plane),
        scratch_shapes=[
            VMEM(snap.shape, jnp.bfloat16),
            VMEM(basis_three.shape, jnp.bfloat16),
            VMEM(basis_two.shape, jnp.bfloat16),
            pltpu.SemaphoreType.DMA((parts + 2,)),
        ],
        compiler_params=pltpu.CompilerParams(vmem_limit_bytes=20 * MIB),
        name="project_three",
    )(*args)


def project_two_kernel(cols, steps, first, *refs):
    recv = refs[:cols]
    if first:
        outs, factor_ref, held = refs[cols:-2], refs[-2], refs[-1]
        cells = recv[0].shape[0] // (steps + 1)
        factor = jnp.concatenate([ref[steps * cells :, :] for ref in recv], axis=0)
        factor = factor.astype(jnp.float32).T.astype(jnp.bfloat16)
        factor_ref[...] = factor
    else:
        recv = recv[cols // 2 :] + recv[: cols // 2]
        factor, outs, held = refs[cols][...], refs[cols + 1 : -1], refs[-1]
        cells = recv[0].shape[0] // steps
    part, ranks_two = outs[0].shape
    me = lax.axis_index("z")
    for t in range(steps):
        inner = jnp.concatenate(
            [ref[t * cells : (t + 1) * cells, :] for ref in recv], axis=0
        )
        held[pl.ds(t, ranks_two, stride=steps), :] = jnp.dot(
            factor, inner, preferred_element_type=jnp.float32
        )
    for s, out in zip(slots(len(outs)), outs):
        base = pl.multiple_of(lax.bitwise_xor(me, s) * part, part)
        out[...] = held[pl.ds(base, part), :].astype(jnp.bfloat16)


def project_two(recv, factor, steps, deep, tiled):
    cols = len(recv)
    first = factor is None
    height, width = recv[0].shape
    cells_two = height // (steps + first)
    part = steps * width // deep
    if not tiled:
        if not first:
            recv = recv[cols // 2 :] + recv[: cols // 2]
        else:
            factor = jnp.concatenate([piece[steps * cells_two :] for piece in recv]).T
        inner = jnp.stack([piece[: steps * cells_two] for piece in recv])
        inner = inner.reshape(cols, steps, cells_two, width)
        full = jnp.einsum(
            "jtbl,qjb->qtl",
            inner,
            factor.reshape(width, cols, cells_two),
            preferred_element_type=jnp.float32,
        )
        full = full.astype(jnp.bfloat16).reshape(deep, part, width)
        return [jnp.take(full, lax.axis_index("z") ^ s, axis=0) for s in slots(deep)], factor
    outs = [jax.ShapeDtypeStruct((part, width), jnp.bfloat16)] * deep
    if first:
        outs.append(jax.ShapeDtypeStruct((width, cols * cells_two), jnp.bfloat16))
    args = recv if first else recv + [factor]
    outs = pl.pallas_call(
        functools.partial(project_two_kernel, cols, steps, first),
        out_shape=outs,
        in_specs=in_vmem(len(args)),
        out_specs=in_vmem(len(outs)),
        scratch_shapes=[VMEM((steps * width, width), jnp.float32)],
        compiler_params=pltpu.CompilerParams(vmem_limit_bytes=20 * MIB),
        name="project_two",
    )(*args)
    return (outs[:deep], outs[deep]) if first else (outs, factor)


def gram_block(left, right):
    return lax.dot_general(
        left, right, (((1,), (1,)), ((), ())), preferred_element_type=jnp.float32
    )


def other_core_gram_kernel(plane, *refs):
    recv, (flat, out) = refs[:-2], refs[-2:]
    deep = len(recv) // 2
    cells_one = flat.shape[0] // (2 * deep)
    halves, _, cells_out = out.shape
    part, width = recv[0].shape
    steps = cells_one // plane
    block = width // plane
    me_z, me_x = lax.axis_index("z"), lax.axis_index("x")
    for side in range(2):
        for n, s in enumerate(slots(deep)):
            ref = recv[side * deep + n]
            row = lax.bitwise_xor(me_z, s) * 2 + lax.bitwise_xor(me_x, side)
            base = pl.multiple_of(row * cells_one, cells_one)
            for u in range(part // steps // plane):
                tiles = ref[u * plane * steps : (u + 1) * plane * steps, :]
                tiles = tiles.astype(jnp.float32)
                tiles = [tiles[q * steps : (q + 1) * steps] for q in range(plane)]
                stacked = jnp.concatenate(swap_blocks(tiles, block), axis=0)
                flat[pl.ds(base, cells_one), u * width : (u + 1) * width] = stacked.astype(
                    jnp.bfloat16
                )
    other = 1 - lax.axis_index("core")
    left = flat[...]
    for y in range(halves):
        base = pl.multiple_of((2 * y + other) * cells_out, cells_out)
        out[y] = gram_block(left, flat[pl.ds(base, cells_out), :])


def own_core_gram_kernel(scale, flat, recv, out):
    halves, _, cells_out = recv.shape
    cells_one = out.shape[1]
    core = lax.axis_index("core")
    left = flat[...]
    for y in range(halves):
        base = pl.multiple_of((2 * y + core) * cells_out, cells_out)
        gram = gram_block(left, flat[pl.ds(base, cells_out), :])
        gram = ((gram + recv[y]) * scale).astype(out.dtype)
        for i in range(out.shape[0] // halves):
            out[i * halves + y] = gram[i * cells_one : (i + 1) * cells_one, :]


def chip_gram(recv, cells_one, plane, scale, tiled):
    deep = len(recv) // 2
    part, width = recv[0].shape
    steps = cells_one // plane
    ranks = part // steps
    block = width // plane
    rows = 2 * deep
    cells = rows * cells_one
    halves = plane // 4
    cells_out = cells // (2 * halves)
    swap = [(0, 1), (1, 0)]
    if not tiled:
        flat = jnp.stack(recv[:deep][::-1] + recv[deep:][::-1])
        flat = flat.reshape(2, deep, ranks, steps, plane, block)
        flat = jnp.take(flat, lax.axis_index("z") ^ jnp.arange(deep), axis=1)
        flat = jnp.take(flat, lax.axis_index("x") ^ jnp.arange(2), axis=0)
        flat = flat.transpose(1, 0, 4, 3, 2, 5).reshape(cells, ranks * block)
        gram = gram_block(flat, flat).reshape(rows, cells_one, halves, 2, cells_out)
        gram = gram.transpose(3, 0, 2, 1, 4).reshape(2, rows * halves, cells_one, cells_out)
        core = lax.axis_index("core")
        sent = lax.ppermute(jnp.take(gram, 1 - core, axis=0), "core", swap)
        return ((jnp.take(gram, core, axis=0) + sent) * scale).astype(jnp.bfloat16)
    params = pltpu.CompilerParams(vmem_limit_bytes=20 * MIB)
    flat, other = pl.pallas_call(
        functools.partial(other_core_gram_kernel, plane),
        out_shape=[
            jax.ShapeDtypeStruct((cells, ranks * block), jnp.bfloat16),
            jax.ShapeDtypeStruct((halves, cells, cells_out), jnp.float32),
        ],
        in_specs=in_vmem(2 * deep),
        out_specs=in_vmem(2),
        compiler_params=params,
        name="other_core_gram",
    )(*recv)
    other = lax.ppermute(other, "core", swap)
    return pl.pallas_call(
        functools.partial(own_core_gram_kernel, scale),
        out_shape=jax.ShapeDtypeStruct((rows * halves, cells_one, cells_out), jnp.bfloat16),
        in_specs=in_vmem(2),
        out_specs=in_vmem(1)[0],
        compiler_params=params,
        name="own_core_gram",
    )(flat, other)


def exchange(pieces, axis, order):
    count = len(pieces)
    assert count & (count - 1) == 0
    return [
        lax.ppermute(piece, axis, [(i, i ^ s) for i in range(count)]) if s else piece
        for s, piece in zip(order, pieces)
    ]


def on_device(deep, cols, snapshot, basis_two, basis_three):
    cells_one = snapshot.shape[0]
    ranks_two, ranks_three = basis_two.shape[1], basis_three.shape[1]
    scale = 1.0 / (ranks_two * ranks_three)
    plane = 2 * cols
    steps = cells_one // plane
    tiled = (
        ranks_two == 128
        and ranks_three == 128
        and steps % 8 == 0
        and ranks_two // deep % plane == 0
        and 2 * deep * cells_one // cols % 128 == 0
    )
    pieces = project_three(snapshot, basis_two, basis_three, plane, cols, tiled)
    pieces = exchange(pieces, PLANE, plane_slots(plane))
    shares, factor = [], None
    for side in (pieces[:cols], pieces[cols:]):
        share, factor = project_two(side, factor, steps, deep, tiled)
        shares += exchange(share, "z", slots(deep))
    parts = chip_gram(shares, cells_one, plane, scale, tiled)
    parts = lax.all_to_all(
        parts, ("z", "x", "y"), split_axis=0, concat_axis=0, tiled=True
    )
    return jnp.sum(parts.astype(jnp.float32), axis=0)


def solution(mesh):
    rows, cols = mesh.shape["row"], mesh.shape["col"]
    devices = mesh.devices.reshape(rows // 2, 2, cols // 2, 2)
    row, col = ("z", "x"), ("y", "core")
    return jax.shard_map(
        functools.partial(on_device, rows // 2, cols),
        mesh=Mesh(devices, row + col),
        in_specs=(P(row, col, None), P(col, None), P()),
        out_specs=P(row, col),
        check_vma=False,
    )
```

```python
import functools

import jax
import jax.numpy as jnp
from jax import lax
from jax.experimental import pallas as pl
from jax.experimental.pallas import tpu as pltpu
from jax.sharding import Mesh
from jax.sharding import PartitionSpec as P

VMEM = pltpu.VMEM
MIB = 1024 * 1024
PLANE = ("x", "y", "core")


def in_vmem(count):
    return [pl.BlockSpec(memory_space=VMEM)] * count


def slots(count):
    return list(reversed(range(count)))


def plane_slots(plane):
    cols = plane // 2
    return slots(cols) + [s ^ (cols // 2) for s in slots(plane)[:cols]]


def place(axes):
    index = 0
    for axis in axes:
        index = index * lax.axis_size(axis) + lax.axis_index(axis)
    return index


def swap_blocks(tiles, width, me=None):
    tiles = list(tiles)
    lane = lax.broadcasted_iota(jnp.int32, tiles[0].shape, 1) // width
    lanes = len(tiles) * width
    step = 1
    while step < len(tiles):
        low = lax.bitwise_and(lane, step) == 0
        for i in range(len(tiles)):
            if i & step:
                continue
            one, two = tiles[i], tiles[i | step]
            zeros = jnp.where(low, one, pltpu.roll(two, step * width, 1))
            ones = jnp.where(low, pltpu.roll(one, lanes - step * width, 1), two)
            if me is None:
                tiles[i], tiles[i | step] = zeros, ones
            else:
                flip = lax.bitwise_and(me, step) != 0
                tiles[i] = jnp.where(flip, ones, zeros)
                tiles[i | step] = jnp.where(flip, zeros, ones)
        step *= 2
    return tiles


def bits(count):
    return [1 << bit for bit in range(count.bit_length() - 1)]


def flip_blocks(tile, width, step):
    lane = lax.broadcasted_iota(jnp.int32, tile.shape, 1) // width
    low = lax.bitwise_and(lane, step) == 0
    lanes = tile.shape[1]
    up = pltpu.roll(tile, step * width, 1)
    return jnp.where(low, pltpu.roll(tile, lanes - step * width, 1), up)


def project_three_kernel(parts, snap, three, two, *rest):
    groups, steps, cells_two, cells_three = snap.shape
    outs = rest[:groups]
    buf, three_buf, two_buf, sems = rest[groups:]
    per = steps // parts
    rows = per * cells_two
    width = three.shape[1] // groups
    me = place(PLANE)
    copies = [
        pltpu.make_async_copy(three, three_buf.at[0], sems.at[parts]),
        pltpu.make_async_copy(two, two_buf, sems.at[parts + 1]),
    ]
    for n in range(parts):
        part = (slice(None), pl.ds(n * per, per))
        copies.append(pltpu.make_async_copy(snap.at[part], buf.at[part], sems.at[n]))
    for copy in copies:
        copy.start()
    copies[0].wait()
    for step in bits(groups):
        for g in range(step):
            tile = three_buf[g].astype(jnp.float32)
            three_buf[g | step] = flip_blocks(tile, width, step).astype(jnp.bfloat16)
    lane = lax.broadcasted_iota(jnp.int32, (rows, three.shape[1]), 1) // width
    keep = {step: lax.bitwise_and(lax.bitwise_xor(lane, me), step) == 0 for step in bits(groups)}
    for n in range(parts):
        copies[2 + n].wait()
        tiles = [
            jnp.dot(
                buf[g, n * per : (n + 1) * per].reshape(rows, cells_three),
                three_buf[g],
                preferred_element_type=jnp.float32,
            )
            for g in range(groups)
        ]
        for step in bits(groups):
            for i in range(groups):
                if i & step == 0:
                    one, two_tile = tiles[i], tiles[i | step]
                    tiles[i] = jnp.where(keep[step], one, two_tile)
                    tiles[i | step] = jnp.where(keep[step], two_tile, one)
        for s, out in zip(plane_slots(groups), outs):
            out[n * rows : (n + 1) * rows, :] = tiles[s].astype(jnp.bfloat16)
    copies[1].wait()
    for out in outs:
        if out.shape[0] > steps * cells_two:
            out[steps * cells_two :, :] = two_buf[...]


def project_three(snapshot, basis_two, basis_three, plane, cols, tiled):
    cells_one, cells_two, cells_three = snapshot.shape
    ranks_three = basis_three.shape[1]
    steps = cells_one // plane
    snap = snapshot.reshape(plane, steps, cells_two, cells_three)
    if not tiled:
        inner = jnp.einsum(
            "gtbc,cr->gtbr", snap, basis_three, preferred_element_type=jnp.float32
        ).astype(jnp.bfloat16)
        inner = inner.reshape(plane, steps, cells_two, plane, ranks_three // plane)
        inner = inner.transpose(3, 1, 2, 0, 4)
        inner = inner.reshape(plane, steps * cells_two, ranks_three)
        pieces = [jnp.take(inner, place(PLANE) ^ s, axis=0) for s in plane_slots(plane)]
        return [
            jnp.concatenate([piece, basis_two]) if s < cols else piece
            for s, piece in zip(plane_slots(plane), pieces)
        ]
    parts = 2
    outs = [
        jax.ShapeDtypeStruct(((steps + (s < cols)) * cells_two, ranks_three), jnp.bfloat16)
        for s in plane_slots(plane)
    ]
    args = [
        pltpu.with_memory_space_constraint(arg, pltpu.HBM)
        for arg in (snap, basis_three, basis_two)
    ]
    return pl.pallas_call(
        functools.partial(project_three_kernel, parts),
        out_shape=outs,
        in_specs=[pl.BlockSpec(memory_space=pltpu.HBM)] * 3,
        out_specs=in_vmem(plane),
        scratch_shapes=[
            VMEM(snap.shape, jnp.bfloat16),
            VMEM((plane,) + basis_three.shape, jnp.bfloat16),
            VMEM(basis_two.shape, jnp.bfloat16),
            pltpu.SemaphoreType.DMA((parts + 2,)),
        ],
        compiler_params=pltpu.CompilerParams(vmem_limit_bytes=20 * MIB),
        name="project_three",
    )(*args)


def project_two_kernel(cols, steps, first, *refs):
    recv = refs[:cols]
    if first:
        outs, factor_ref, held = refs[cols:-2], refs[-2], refs[-1]
        cells = recv[0].shape[0] // (steps + 1)
        factor = jnp.concatenate([ref[steps * cells :, :] for ref in recv], axis=0)
        factor = factor.astype(jnp.float32).T.astype(jnp.bfloat16)
        factor_ref[...] = factor
    else:
        recv = recv[cols // 2 :] + recv[: cols // 2]
        factor, outs, held = refs[cols][...], refs[cols + 1 : -1], refs[-1]
        cells = recv[0].shape[0] // steps
    part, ranks_two = outs[0].shape
    me = lax.axis_index("z")
    for t in range(steps):
        inner = jnp.concatenate(
            [ref[t * cells : (t + 1) * cells, :] for ref in recv], axis=0
        )
        held[pl.ds(t, ranks_two, stride=steps), :] = jnp.dot(
            factor, inner, preferred_element_type=jnp.float32
        )
    for s, out in zip(slots(len(outs)), outs):
        base = pl.multiple_of(lax.bitwise_xor(me, s) * part, part)
        out[...] = held[pl.ds(base, part), :].astype(jnp.bfloat16)


def project_two(recv, factor, steps, deep, tiled):
    cols = len(recv)
    first = factor is None
    height, width = recv[0].shape
    cells_two = height // (steps + first)
    part = steps * width // deep
    if not tiled:
        if not first:
            recv = recv[cols // 2 :] + recv[: cols // 2]
        else:
            factor = jnp.concatenate([piece[steps * cells_two :] for piece in recv]).T
        inner = jnp.stack([piece[: steps * cells_two] for piece in recv])
        inner = inner.reshape(cols, steps, cells_two, width)
        full = jnp.einsum(
            "jtbl,qjb->qtl",
            inner,
            factor.reshape(width, cols, cells_two),
            preferred_element_type=jnp.float32,
        )
        full = full.astype(jnp.bfloat16).reshape(deep, part, width)
        return [jnp.take(full, lax.axis_index("z") ^ s, axis=0) for s in slots(deep)], factor
    outs = [jax.ShapeDtypeStruct((part, width), jnp.bfloat16)] * deep
    if first:
        outs.append(jax.ShapeDtypeStruct((width, cols * cells_two), jnp.bfloat16))
    args = recv if first else recv + [factor]
    outs = pl.pallas_call(
        functools.partial(project_two_kernel, cols, steps, first),
        out_shape=outs,
        in_specs=in_vmem(len(args)),
        out_specs=in_vmem(len(outs)),
        scratch_shapes=[VMEM((steps * width, width), jnp.float32)],
        compiler_params=pltpu.CompilerParams(vmem_limit_bytes=20 * MIB),
        name="project_two",
    )(*args)
    return (outs[:deep], outs[deep]) if first else (outs, factor)


def gram_block(left, right):
    return lax.dot_general(
        left, right, (((1,), (1,)), ((), ())), preferred_element_type=jnp.float32
    )


def fill_side(plane, side, recv, flat):
    deep = len(recv)
    cells_one = flat.shape[0] // (2 * deep)
    part, width = recv[0].shape
    steps = cells_one // plane
    me_z, me_x = lax.axis_index("z"), lax.axis_index("x")
    for s, ref in zip(slots(deep), recv):
        row = lax.bitwise_xor(me_z, s) * 2 + lax.bitwise_xor(me_x, side)
        base = pl.multiple_of(row * cells_one, cells_one)
        for u in range(part // steps // plane):
            tiles = ref[u * plane * steps : (u + 1) * plane * steps, :].astype(jnp.float32)
            tiles = [tiles[q * steps : (q + 1) * steps] for q in range(plane)]
            stacked = jnp.concatenate(swap_blocks(tiles, width // plane, place(PLANE)), axis=0)
            flat[pl.ds(base, cells_one), u * width : (u + 1) * width] = stacked.astype(
                jnp.bfloat16
            )


def first_side_kernel(plane, *refs):
    fill_side(plane, 0, refs[:-1], refs[-1])


def other_core_gram_kernel(plane, *refs):
    recv, (half, flat, out) = refs[:-3], refs[-3:]
    halves, _, cells_out = out.shape
    fill_side(plane, 1, recv, flat)
    other = 1 - lax.axis_index("core")
    left = flat[...]
    for y in range(halves):
        base = pl.multiple_of((2 * y + other) * cells_out, cells_out)
        out[y] = gram_block(left, flat[pl.ds(base, cells_out), :])


def own_core_gram_kernel(scale, flat, recv, out):
    halves, _, cells_out = recv.shape
    cells_one = out.shape[1]
    core = lax.axis_index("core")
    left = flat[...]
    for y in range(halves):
        base = pl.multiple_of((2 * y + core) * cells_out, cells_out)
        gram = gram_block(left, flat[pl.ds(base, cells_out), :])
        gram = ((gram + recv[y]) * scale).astype(out.dtype)
        for i in range(out.shape[0] // halves):
            out[i * halves + y] = gram[i * cells_one : (i + 1) * cells_one, :]


def chip_gram(recv, cells_one, plane, scale, tiled):
    deep = len(recv) // 2
    part, width = recv[0].shape
    steps = cells_one // plane
    ranks = part // steps
    block = width // plane
    rows = 2 * deep
    cells = rows * cells_one
    halves = plane // 4
    cells_out = cells // (2 * halves)
    swap = [(0, 1), (1, 0)]
    if not tiled:
        flat = jnp.stack(recv[:deep][::-1] + recv[deep:][::-1])
        flat = flat.reshape(2, deep, ranks, steps, plane, block)
        flat = jnp.take(flat, lax.axis_index("z") ^ jnp.arange(deep), axis=1)
        flat = jnp.take(flat, lax.axis_index("x") ^ jnp.arange(2), axis=0)
        flat = flat.transpose(1, 0, 4, 3, 2, 5).reshape(cells, ranks * block)
        gram = gram_block(flat, flat).reshape(rows, cells_one, halves, 2, cells_out)
        gram = gram.transpose(3, 0, 2, 1, 4).reshape(2, rows * halves, cells_one, cells_out)
        core = lax.axis_index("core")
        sent = lax.ppermute(jnp.take(gram, 1 - core, axis=0), "core", swap)
        return ((jnp.take(gram, core, axis=0) + sent) * scale).astype(jnp.bfloat16)
    params = pltpu.CompilerParams(vmem_limit_bytes=20 * MIB)
    flat = jax.ShapeDtypeStruct((cells, ranks * block), jnp.bfloat16)
    half = pl.pallas_call(
        functools.partial(first_side_kernel, plane),
        out_shape=flat,
        in_specs=in_vmem(deep),
        out_specs=in_vmem(1)[0],
        compiler_params=params,
        name="first_side",
    )(*recv[:deep])
    flat, other = pl.pallas_call(
        functools.partial(other_core_gram_kernel, plane),
        out_shape=[flat, jax.ShapeDtypeStruct((halves, cells, cells_out), jnp.float32)],
        in_specs=in_vmem(deep + 1),
        out_specs=in_vmem(2),
        input_output_aliases={deep: 0},
        compiler_params=params,
        name="other_core_gram",
    )(*recv[deep:], half)
    other = lax.ppermute(other, "core", swap)
    return pl.pallas_call(
        functools.partial(own_core_gram_kernel, scale),
        out_shape=jax.ShapeDtypeStruct((rows * halves, cells_one, cells_out), jnp.bfloat16),
        in_specs=in_vmem(2),
        out_specs=in_vmem(1)[0],
        compiler_params=params,
        name="own_core_gram",
    )(flat, other)


def exchange(pieces, axis, order):
    count = len(pieces)
    assert count & (count - 1) == 0
    return [
        lax.ppermute(piece, axis, [(i, i ^ s) for i in range(count)]) if s else piece
        for s, piece in zip(order, pieces)
    ]


def on_device(deep, cols, snapshot, basis_two, basis_three):
    cells_one = snapshot.shape[0]
    ranks_two, ranks_three = basis_two.shape[1], basis_three.shape[1]
    scale = 1.0 / (ranks_two * ranks_three)
    plane = 2 * cols
    steps = cells_one // plane
    tiled = (
        ranks_two == 128
        and ranks_three == 128
        and steps % 8 == 0
        and ranks_two // deep % plane == 0
        and 2 * deep * cells_one // cols % 128 == 0
    )
    pieces = project_three(snapshot, basis_two, basis_three, plane, cols, tiled)
    pieces = exchange(pieces, PLANE, plane_slots(plane))
    shares, factor = [], None
    for side in (pieces[:cols], pieces[cols:]):
        share, factor = project_two(side, factor, steps, deep, tiled)
        shares += exchange(share, "z", slots(deep))
    parts = chip_gram(shares, cells_one, plane, scale, tiled)
    parts = lax.all_to_all(
        parts, ("z", "x", "y"), split_axis=0, concat_axis=0, tiled=True
    )
    return jnp.sum(parts.astype(jnp.float32), axis=0)


def solution(mesh):
    rows, cols = mesh.shape["row"], mesh.shape["col"]
    devices = mesh.devices.reshape(rows // 2, 2, cols // 2, 2)
    row, col = ("z", "x"), ("y", "core")
    return jax.shard_map(
        functools.partial(on_device, rows // 2, cols),
        mesh=Mesh(devices, row + col),
        in_specs=(P(row, col, None), P(col, None), P()),
        out_specs=P(row, col),
        check_vma=False,
    )
```

```python
import functools

import jax
import jax.numpy as jnp
from jax import lax
from jax.experimental import pallas as pl
from jax.experimental.pallas import tpu as pltpu
from jax.sharding import Mesh
from jax.sharding import PartitionSpec as P

VMEM = pltpu.VMEM
MIB = 1024 * 1024
PLANE = ("x", "y", "core")


def in_vmem(count):
    return [pl.BlockSpec(memory_space=VMEM)] * count


def slots(count):
    return list(reversed(range(count)))


def plane_slots(plane):
    cols = plane // 2
    return slots(cols) + [s ^ (cols // 2) for s in slots(plane)[:cols]]


def place(axes):
    index = 0
    for axis in axes:
        index = index * lax.axis_size(axis) + lax.axis_index(axis)
    return index


def swap_blocks(tiles, width, me=None):
    tiles = list(tiles)
    lane = lax.broadcasted_iota(jnp.int32, tiles[0].shape, 1) // width
    lanes = len(tiles) * width
    step = 1
    while step < len(tiles):
        low = lax.bitwise_and(lane, step) == 0
        for i in range(len(tiles)):
            if i & step:
                continue
            one, two = tiles[i], tiles[i | step]
            zeros = jnp.where(low, one, pltpu.roll(two, step * width, 1))
            ones = jnp.where(low, pltpu.roll(one, lanes - step * width, 1), two)
            if me is None:
                tiles[i], tiles[i | step] = zeros, ones
            else:
                flip = lax.bitwise_and(me, step) != 0
                tiles[i] = jnp.where(flip, ones, zeros)
                tiles[i | step] = jnp.where(flip, zeros, ones)
        step *= 2
    return tiles


def bits(count):
    return [1 << bit for bit in range(count.bit_length() - 1)]


def flip_blocks(tile, width, step):
    lane = lax.broadcasted_iota(jnp.int32, tile.shape, 1) // width
    low = lax.bitwise_and(lane, step) == 0
    lanes = tile.shape[1]
    up = pltpu.roll(tile, step * width, 1)
    return jnp.where(low, pltpu.roll(tile, lanes - step * width, 1), up)


def project_three_kernel(parts, snap, three, two, *rest):
    groups, steps, cells_two, cells_three = snap.shape
    outs = rest[:groups]
    buf, three_buf, two_buf, sems = rest[groups:]
    per = steps // parts
    rows = per * cells_two
    width = three.shape[1] // groups
    me = place(PLANE)
    copies = [
        pltpu.make_async_copy(three, three_buf.at[0], sems.at[parts]),
        pltpu.make_async_copy(two, two_buf, sems.at[parts + 1]),
    ]
    for n in range(parts):
        part = (slice(None), pl.ds(n * per, per))
        copies.append(pltpu.make_async_copy(snap.at[part], buf.at[part], sems.at[n]))
    for copy in copies:
        copy.start()
    copies[0].wait()
    for step in bits(groups):
        for g in range(step):
            tile = three_buf[g].astype(jnp.float32)
            three_buf[g | step] = flip_blocks(tile, width, step).astype(jnp.bfloat16)
    lane = lax.broadcasted_iota(jnp.int32, (rows, three.shape[1]), 1) // width
    keep = {step: lax.bitwise_and(lax.bitwise_xor(lane, me), step) == 0 for step in bits(groups)}
    for n in range(parts):
        copies[2 + n].wait()
        tiles = [
            jnp.dot(
                buf[g, n * per : (n + 1) * per].reshape(rows, cells_three),
                three_buf[g],
                preferred_element_type=jnp.float32,
            )
            for g in range(groups)
        ]
        for step in bits(groups):
            for i in range(groups):
                if i & step == 0:
                    one, two_tile = tiles[i], tiles[i | step]
                    tiles[i] = jnp.where(keep[step], one, two_tile)
                    tiles[i | step] = jnp.where(keep[step], two_tile, one)
        for s, out in zip(plane_slots(groups), outs):
            out[n * rows : (n + 1) * rows, :] = tiles[s].astype(jnp.bfloat16)
    copies[1].wait()
    for out in outs:
        if out.shape[0] > steps * cells_two:
            out[steps * cells_two :, :] = two_buf[...]


def project_three(snapshot, basis_two, basis_three, plane, cols, tiled):
    cells_one, cells_two, cells_three = snapshot.shape
    ranks_three = basis_three.shape[1]
    steps = cells_one // plane
    snap = snapshot.reshape(plane, steps, cells_two, cells_three)
    if not tiled:
        inner = jnp.einsum(
            "gtbc,cr->gtbr", snap, basis_three, preferred_element_type=jnp.float32
        ).astype(jnp.bfloat16)
        inner = inner.reshape(plane, steps, cells_two, plane, ranks_three // plane)
        inner = inner.transpose(3, 1, 2, 0, 4)
        inner = inner.reshape(plane, steps * cells_two, ranks_three)
        pieces = [jnp.take(inner, place(PLANE) ^ s, axis=0) for s in plane_slots(plane)]
        return [
            jnp.concatenate([piece, basis_two]) if s < cols else piece
            for s, piece in zip(plane_slots(plane), pieces)
        ]
    parts = 2
    outs = [
        jax.ShapeDtypeStruct(((steps + (s < cols)) * cells_two, ranks_three), jnp.bfloat16)
        for s in plane_slots(plane)
    ]
    args = [
        pltpu.with_memory_space_constraint(arg, pltpu.HBM)
        for arg in (snap, basis_three, basis_two)
    ]
    return pl.pallas_call(
        functools.partial(project_three_kernel, parts),
        out_shape=outs,
        in_specs=[pl.BlockSpec(memory_space=pltpu.HBM)] * 3,
        out_specs=in_vmem(plane),
        scratch_shapes=[
            VMEM(snap.shape, jnp.bfloat16),
            VMEM((plane,) + basis_three.shape, jnp.bfloat16),
            VMEM(basis_two.shape, jnp.bfloat16),
            pltpu.SemaphoreType.DMA((parts + 2,)),
        ],
        compiler_params=pltpu.CompilerParams(vmem_limit_bytes=20 * MIB),
        name="project_three",
    )(*args)


def project_two_kernel(cols, steps, first, *refs):
    recv = refs[:cols]
    if first:
        outs, factor_ref, held = refs[cols:-2], refs[-2], refs[-1]
        cells = recv[0].shape[0] // (steps + 1)
        factor = jnp.concatenate([ref[steps * cells :, :] for ref in recv], axis=0)
        factor = factor.astype(jnp.float32).T.astype(jnp.bfloat16)
        factor_ref[...] = factor
    else:
        recv = recv[cols // 2 :] + recv[: cols // 2]
        factor, outs, held = refs[cols][...], refs[cols + 1 : -1], refs[-1]
        cells = recv[0].shape[0] // steps
    part, ranks_two = outs[0].shape
    me = lax.axis_index("z")
    for t in range(steps):
        inner = jnp.concatenate(
            [ref[t * cells : (t + 1) * cells, :] for ref in recv], axis=0
        )
        held[pl.ds(t, ranks_two, stride=steps), :] = jnp.dot(
            factor, inner, preferred_element_type=jnp.float32
        )
    for s, out in zip(slots(len(outs)), outs):
        base = pl.multiple_of(lax.bitwise_xor(me, s) * part, part)
        out[...] = held[pl.ds(base, part), :].astype(jnp.bfloat16)


def project_two(recv, factor, steps, deep, tiled):
    cols = len(recv)
    first = factor is None
    height, width = recv[0].shape
    cells_two = height // (steps + first)
    part = steps * width // deep
    if not tiled:
        if not first:
            recv = recv[cols // 2 :] + recv[: cols // 2]
        else:
            factor = jnp.concatenate([piece[steps * cells_two :] for piece in recv]).T
        inner = jnp.stack([piece[: steps * cells_two] for piece in recv])
        inner = inner.reshape(cols, steps, cells_two, width)
        full = jnp.einsum(
            "jtbl,qjb->qtl",
            inner,
            factor.reshape(width, cols, cells_two),
            preferred_element_type=jnp.float32,
        )
        full = full.astype(jnp.bfloat16).reshape(deep, part, width)
        return [jnp.take(full, lax.axis_index("z") ^ s, axis=0) for s in slots(deep)], factor
    outs = [jax.ShapeDtypeStruct((part, width), jnp.bfloat16)] * deep
    if first:
        outs.append(jax.ShapeDtypeStruct((width, cols * cells_two), jnp.bfloat16))
    args = recv if first else recv + [factor]
    outs = pl.pallas_call(
        functools.partial(project_two_kernel, cols, steps, first),
        out_shape=outs,
        in_specs=in_vmem(len(args)),
        out_specs=in_vmem(len(outs)),
        scratch_shapes=[VMEM((steps * width, width), jnp.float32)],
        compiler_params=pltpu.CompilerParams(vmem_limit_bytes=20 * MIB),
        name="project_two",
    )(*args)
    return (outs[:deep], outs[deep]) if first else (outs, factor)


def gram_block(left, right):
    return lax.dot_general(
        left, right, (((1,), (1,)), ((), ())), preferred_element_type=jnp.float32
    )


def fill_side(plane, side, recv, flat):
    deep = len(recv)
    cells_one = flat.shape[0] // (2 * deep)
    part, width = recv[0].shape
    steps = cells_one // plane
    me_z, me_x = lax.axis_index("z"), lax.axis_index("x")
    for s, ref in zip(slots(deep), recv):
        row = lax.bitwise_xor(me_z, s) * 2 + lax.bitwise_xor(me_x, side)
        base = pl.multiple_of(row * cells_one, cells_one)
        for u in range(part // steps // plane):
            tiles = ref[u * plane * steps : (u + 1) * plane * steps, :].astype(jnp.float32)
            tiles = [tiles[q * steps : (q + 1) * steps] for q in range(plane)]
            stacked = jnp.concatenate(swap_blocks(tiles, width // plane, place(PLANE)), axis=0)
            flat[pl.ds(base, cells_one), u * width : (u + 1) * width] = stacked.astype(
                jnp.bfloat16
            )


def first_side_kernel(plane, *refs):
    fill_side(plane, 0, refs[:-1], refs[-1])


def chip_block(flat, slot, core, cells_out):
    halves = lax.axis_size("y")
    deep = lax.axis_size("z")
    cells_one = flat.shape[0] // (2 * deep)
    where = lax.bitwise_xor(place(("x", "y")), slot)
    x, y = where // halves, lax.rem(where, halves)
    left = [
        flat[pl.ds(pl.multiple_of((2 * z + x) * cells_one, cells_one), cells_one), :]
        for z in range(deep)
    ]
    base = pl.multiple_of((2 * y + core) * cells_out, cells_out)
    return gram_block(jnp.concatenate(left, axis=0), flat[pl.ds(base, cells_out), :])


def other_core_gram_kernel(plane, *refs):
    recv, (half, flat, out) = refs[:-3], refs[-3:]
    fill_side(plane, 1, recv, flat)
    core = 1 - lax.axis_index("core")
    for s in range(out.shape[0]):
        out[s] = chip_block(flat, s, core, out.shape[2])


def own_core_gram_kernel(scale, flat, recv, *outs):
    core = lax.axis_index("core")
    for s, out in zip(slots(len(outs)), outs):
        gram = chip_block(flat, s, core, out.shape[1]) + recv[s]
        out[...] = (gram * scale).astype(out.dtype)


def chip_sum_kernel(chips, *refs):
    recv, outs, total = refs[:chips], refs[chips:-1], refs[-1]
    acc = recv[-1][...]
    for ref in recv[:-1]:
        acc = acc + ref[...].astype(jnp.float32)
    total[...] = acc
    rows = outs[0].shape[0]
    me = lax.axis_index("z")
    for s, out in zip(slots(len(outs)), outs):
        base = pl.multiple_of(lax.bitwise_xor(me, s) * rows, rows)
        out[...] = total[pl.ds(base, rows), :]


def gram(recv, cells_one, plane, scale, tiled):
    deep = len(recv) // 2
    part, width = recv[0].shape
    steps = cells_one // plane
    ranks = part // steps
    block = width // plane
    rows = 2 * deep
    cells = rows * cells_one
    halves = plane // 4
    cells_out = cells // (2 * halves)
    swap = [(0, 1), (1, 0)]
    if not tiled:
        flat = jnp.stack(recv[:deep][::-1] + recv[deep:][::-1])
        flat = flat.reshape(2, deep, ranks, steps, plane, block)
        flat = jnp.take(flat, lax.axis_index("z") ^ jnp.arange(deep), axis=1)
        flat = jnp.take(flat, lax.axis_index("x") ^ jnp.arange(2), axis=0)
        flat = flat.transpose(1, 0, 4, 3, 2, 5).reshape(cells, ranks * block)
        whole = gram_block(flat, flat).reshape(rows, cells_one, halves, 2, cells_out)
        whole = whole.transpose(3, 0, 2, 1, 4).reshape(2, rows * halves, cells_one, cells_out)
        core = lax.axis_index("core")
        sent = lax.ppermute(jnp.take(whole, 1 - core, axis=0), "core", swap)
        parts = ((jnp.take(whole, core, axis=0) + sent) * scale).astype(jnp.bfloat16)
        parts = lax.all_to_all(
            parts, ("z", "x", "y"), split_axis=0, concat_axis=0, tiled=True
        )
        return jnp.sum(parts.astype(jnp.float32), axis=0)
    params = pltpu.CompilerParams(vmem_limit_bytes=20 * MIB)
    chips = 2 * halves
    flat = jax.ShapeDtypeStruct((cells, ranks * block), jnp.bfloat16)
    half = pl.pallas_call(
        functools.partial(first_side_kernel, plane),
        out_shape=flat,
        in_specs=in_vmem(deep),
        out_specs=in_vmem(1)[0],
        compiler_params=params,
        name="first_side",
    )(*recv[:deep])
    flat, other = pl.pallas_call(
        functools.partial(other_core_gram_kernel, plane),
        out_shape=[flat, jax.ShapeDtypeStruct((chips, cells // 2, cells_out), jnp.float32)],
        in_specs=in_vmem(deep + 1),
        out_specs=in_vmem(2),
        input_output_aliases={deep: 0},
        compiler_params=params,
        name="other_core_gram",
    )(*recv[deep:], half)
    other = lax.ppermute(other, "core", swap)
    sent = jax.ShapeDtypeStruct((cells // 2, cells_out), jnp.bfloat16)
    kept = jax.ShapeDtypeStruct((cells // 2, cells_out), jnp.float32)
    parts = pl.pallas_call(
        functools.partial(own_core_gram_kernel, scale),
        out_shape=[sent] * (chips - 1) + [kept],
        in_specs=in_vmem(2),
        out_specs=in_vmem(chips),
        compiler_params=params,
        name="own_core_gram",
    )(flat, other)
    parts = exchange(parts, ("x", "y"), slots(chips))
    parts = pl.pallas_call(
        functools.partial(chip_sum_kernel, chips),
        out_shape=[jax.ShapeDtypeStruct((cells_one, cells_out), jnp.float32)] * deep,
        in_specs=in_vmem(chips),
        out_specs=in_vmem(deep),
        scratch_shapes=[VMEM((cells // 2, cells_out), jnp.float32)],
        compiler_params=params,
        name="chip_sum",
    )(*parts)
    return sum(exchange(parts, "z", slots(deep)))


def exchange(pieces, axis, order):
    count = len(pieces)
    assert count & (count - 1) == 0
    return [
        lax.ppermute(piece, axis, [(i, i ^ s) for i in range(count)]) if s else piece
        for s, piece in zip(order, pieces)
    ]


def on_device(deep, cols, snapshot, basis_two, basis_three):
    cells_one = snapshot.shape[0]
    ranks_two, ranks_three = basis_two.shape[1], basis_three.shape[1]
    scale = 1.0 / (ranks_two * ranks_three)
    plane = 2 * cols
    steps = cells_one // plane
    tiled = (
        ranks_two == 128
        and ranks_three == 128
        and steps % 8 == 0
        and ranks_two // deep % plane == 0
        and 2 * deep * cells_one // cols % 128 == 0
    )
    pieces = project_three(snapshot, basis_two, basis_three, plane, cols, tiled)
    pieces = exchange(pieces, PLANE, plane_slots(plane))
    shares, factor = [], None
    for side in (pieces[:cols], pieces[cols:]):
        share, factor = project_two(side, factor, steps, deep, tiled)
        shares += exchange(share, "z", slots(deep))
    return gram(shares, cells_one, plane, scale, tiled)


def solution(mesh):
    rows, cols = mesh.shape["row"], mesh.shape["col"]
    devices = mesh.devices.reshape(rows // 2, 2, cols // 2, 2)
    row, col = ("z", "x"), ("y", "core")
    return jax.shard_map(
        functools.partial(on_device, rows // 2, cols),
        mesh=Mesh(devices, row + col),
        in_specs=(P(row, col, None), P(col, None), P()),
        out_specs=P(row, col),
        check_vma=False,
    )
```

```python
import functools

import jax
import jax.numpy as jnp
from jax import lax
from jax.experimental import pallas as pl
from jax.experimental.pallas import tpu as pltpu
from jax.sharding import Mesh
from jax.sharding import PartitionSpec as P

VMEM = pltpu.VMEM
MIB = 1024 * 1024
PLANE = ("x", "y", "core")


def in_vmem(count):
    return [pl.BlockSpec(memory_space=VMEM)] * count


def slots(count):
    return list(reversed(range(count)))


def plane_slots(plane):
    cols = plane // 2
    return slots(cols) + list(range(cols, plane))


def place(axes):
    index = 0
    for axis in axes:
        index = index * lax.axis_size(axis) + lax.axis_index(axis)
    return index


def swap_blocks(tiles, width, me=None):
    tiles = list(tiles)
    lane = lax.broadcasted_iota(jnp.int32, tiles[0].shape, 1) // width
    lanes = len(tiles) * width
    step = 1
    while step < len(tiles):
        low = lax.bitwise_and(lane, step) == 0
        for i in range(len(tiles)):
            if i & step:
                continue
            one, two = tiles[i], tiles[i | step]
            zeros = jnp.where(low, one, pltpu.roll(two, step * width, 1))
            ones = jnp.where(low, pltpu.roll(one, lanes - step * width, 1), two)
            if me is None:
                tiles[i], tiles[i | step] = zeros, ones
            else:
                flip = lax.bitwise_and(me, step) != 0
                tiles[i] = jnp.where(flip, ones, zeros)
                tiles[i | step] = jnp.where(flip, zeros, ones)
        step *= 2
    return tiles


def bits(count):
    return [1 << bit for bit in range(count.bit_length() - 1)]


def flip_blocks(tile, width, step):
    lane = lax.broadcasted_iota(jnp.int32, tile.shape, 1) // width
    low = lax.bitwise_and(lane, step) == 0
    lanes = tile.shape[1]
    up = pltpu.roll(tile, step * width, 1)
    if 2 * step * width == lanes:
        return up
    return jnp.where(low, pltpu.roll(tile, lanes - step * width, 1), up)


def project_three_kernel(parts, snap, three, two, *rest):
    groups, steps, cells_two, cells_three = snap.shape
    outs = rest[:groups]
    buf, three_buf, two_buf, sems = rest[groups:]
    per = steps // parts
    rows = per * cells_two
    width = three.shape[1] // groups
    me = place(PLANE)
    copies = [
        pltpu.make_async_copy(three, three_buf.at[0], sems.at[parts]),
        pltpu.make_async_copy(two, two_buf, sems.at[parts + 1]),
    ]
    for n in range(parts):
        part = (slice(None), pl.ds(n * per, per))
        copies.append(pltpu.make_async_copy(snap.at[part], buf.at[part], sems.at[n]))
    for copy in copies:
        copy.start()
    copies[0].wait()
    for step in bits(groups):
        for g in range(step):
            tile = three_buf[g].astype(jnp.float32)
            three_buf[g | step] = flip_blocks(tile, width, step).astype(jnp.bfloat16)
    lane = lax.broadcasted_iota(jnp.int32, (rows, three.shape[1]), 1) // width
    keep = {step: lax.bitwise_and(lax.bitwise_xor(lane, me), step) == 0 for step in bits(groups)}
    for n in range(parts):
        copies[2 + n].wait()
        tiles = [
            jnp.dot(
                buf[g, n * per : (n + 1) * per].reshape(rows, cells_three),
                three_buf[g],
                preferred_element_type=jnp.float32,
            )
            for g in range(groups)
        ]
        for step in bits(groups):
            for i in range(groups):
                if i & step == 0:
                    one, two_tile = tiles[i], tiles[i | step]
                    tiles[i] = jnp.where(keep[step], one, two_tile)
                    tiles[i | step] = jnp.where(keep[step], two_tile, one)
        for s, out in zip(plane_slots(groups), outs):
            out[n * rows : (n + 1) * rows, :] = tiles[s].astype(jnp.bfloat16)
    copies[1].wait()
    for out in outs:
        if out.shape[0] > steps * cells_two:
            out[steps * cells_two :, :] = two_buf[...]


def project_three(snapshot, basis_two, basis_three, plane, cols, tiled):
    cells_one, cells_two, cells_three = snapshot.shape
    ranks_three = basis_three.shape[1]
    steps = cells_one // plane
    snap = snapshot.reshape(plane, steps, cells_two, cells_three)
    if not tiled:
        inner = jnp.einsum(
            "gtbc,cr->gtbr", snap, basis_three, preferred_element_type=jnp.float32
        ).astype(jnp.bfloat16)
        inner = inner.reshape(plane, steps, cells_two, plane, ranks_three // plane)
        inner = inner.transpose(3, 1, 2, 0, 4)
        inner = inner.reshape(plane, steps * cells_two, ranks_three)
        pieces = [jnp.take(inner, place(PLANE) ^ s, axis=0) for s in plane_slots(plane)]
        return [
            jnp.concatenate([piece, basis_two]) if s < cols else piece
            for s, piece in zip(plane_slots(plane), pieces)
        ]
    parts = 2
    outs = [
        jax.ShapeDtypeStruct(((steps + (s < cols)) * cells_two, ranks_three), jnp.bfloat16)
        for s in plane_slots(plane)
    ]
    args = [
        pltpu.with_memory_space_constraint(arg, pltpu.HBM)
        for arg in (snap, basis_three, basis_two)
    ]
    return pl.pallas_call(
        functools.partial(project_three_kernel, parts),
        out_shape=outs,
        in_specs=[pl.BlockSpec(memory_space=pltpu.HBM)] * 3,
        out_specs=in_vmem(plane),
        scratch_shapes=[
            VMEM(snap.shape, jnp.bfloat16),
            VMEM((plane,) + basis_three.shape, jnp.bfloat16),
            VMEM(basis_two.shape, jnp.bfloat16),
            pltpu.SemaphoreType.DMA((parts + 2,)),
        ],
        compiler_params=pltpu.CompilerParams(vmem_limit_bytes=20 * MIB),
        name="project_three",
    )(*args)


def project_two_kernel(cols, steps, first, *refs):
    recv = refs[:cols]
    if first:
        outs, factor_ref, held = refs[cols:-2], refs[-2], refs[-1]
        cells = recv[0].shape[0] // (steps + 1)
        factor = jnp.concatenate([ref[steps * cells :, :] for ref in recv], axis=0)
        factor = factor.astype(jnp.float32).T.astype(jnp.bfloat16)
        factor_ref[...] = factor
    else:
        recv = recv[::-1]
        factor, outs, held = refs[cols][...], refs[cols + 1 : -1], refs[-1]
        cells = recv[0].shape[0] // steps
    part, ranks_two = outs[0].shape
    me = lax.axis_index("z")
    for t in range(steps):
        inner = jnp.concatenate(
            [ref[t * cells : (t + 1) * cells, :] for ref in recv], axis=0
        )
        held[pl.ds(t, ranks_two, stride=steps), :] = jnp.dot(
            factor, inner, preferred_element_type=jnp.float32
        )
    for s, out in zip(slots(len(outs)), outs):
        base = pl.multiple_of(lax.bitwise_xor(me, s) * part, part)
        out[...] = held[pl.ds(base, part), :].astype(jnp.bfloat16)


def project_two(recv, factor, steps, deep, tiled):
    cols = len(recv)
    first = factor is None
    height, width = recv[0].shape
    cells_two = height // (steps + first)
    part = steps * width // deep
    if not tiled:
        if not first:
            recv = recv[::-1]
        else:
            factor = jnp.concatenate([piece[steps * cells_two :] for piece in recv]).T
        inner = jnp.stack([piece[: steps * cells_two] for piece in recv])
        inner = inner.reshape(cols, steps, cells_two, width)
        full = jnp.einsum(
            "jtbl,qjb->qtl",
            inner,
            factor.reshape(width, cols, cells_two),
            preferred_element_type=jnp.float32,
        )
        full = full.astype(jnp.bfloat16).reshape(deep, part, width)
        return [jnp.take(full, lax.axis_index("z") ^ s, axis=0) for s in slots(deep)], factor
    outs = [jax.ShapeDtypeStruct((part, width), jnp.bfloat16)] * deep
    if first:
        outs.append(jax.ShapeDtypeStruct((width, cols * cells_two), jnp.bfloat16))
    args = recv if first else recv + [factor]
    outs = pl.pallas_call(
        functools.partial(project_two_kernel, cols, steps, first),
        out_shape=outs,
        in_specs=in_vmem(len(args)),
        out_specs=in_vmem(len(outs)),
        scratch_shapes=[VMEM((steps * width, width), jnp.float32)],
        compiler_params=pltpu.CompilerParams(vmem_limit_bytes=20 * MIB),
        name="project_two",
    )(*args)
    return (outs[:deep], outs[deep]) if first else (outs, factor)


def gram_block(left, right):
    return lax.dot_general(
        left, right, (((1,), (1,)), ((), ())), preferred_element_type=jnp.float32
    )


def fill_side(plane, side, recv, flat):
    deep = len(recv)
    cells_one = flat.shape[0] // (2 * deep)
    part, width = recv[0].shape
    steps = cells_one // plane
    me_z, me_x = lax.axis_index("z"), lax.axis_index("x")
    for s, ref in zip(slots(deep), recv):
        row = lax.bitwise_xor(me_z, s) * 2 + lax.bitwise_xor(me_x, side)
        base = pl.multiple_of(row * cells_one, cells_one)
        for u in range(part // steps // plane):
            tiles = ref[u * plane * steps : (u + 1) * plane * steps, :].astype(jnp.float32)
            tiles = [tiles[q * steps : (q + 1) * steps] for q in range(plane)]
            stacked = jnp.concatenate(swap_blocks(tiles, width // plane, place(PLANE)), axis=0)
            flat[pl.ds(base, cells_one), u * width : (u + 1) * width] = stacked.astype(
                jnp.bfloat16
            )


def first_side_kernel(plane, *refs):
    fill_side(plane, 0, refs[:-1], refs[-1])


def chip_block(flat, slot, core, cells_out):
    halves = lax.axis_size("y")
    deep = lax.axis_size("z")
    cells_one = flat.shape[0] // (2 * deep)
    where = lax.bitwise_xor(place(("x", "y")), slot)
    x, y = where // halves, lax.rem(where, halves)
    left = [
        flat[pl.ds(pl.multiple_of((2 * z + x) * cells_one, cells_one), cells_one), :]
        for z in range(deep)
    ]
    base = pl.multiple_of((2 * y + core) * cells_out, cells_out)
    return gram_block(jnp.concatenate(left, axis=0), flat[pl.ds(base, cells_out), :])


def other_core_gram_kernel(plane, *refs):
    recv, (half, flat, out) = refs[:-3], refs[-3:]
    fill_side(plane, 1, recv, flat)
    core = 1 - lax.axis_index("core")
    for s in range(out.shape[0]):
        out[s] = chip_block(flat, s, core, out.shape[2])


def own_core_gram_kernel(scale, flat, recv, *outs):
    core = lax.axis_index("core")
    for s, out in zip(slots(len(outs)), outs):
        gram = chip_block(flat, s, core, out.shape[1]) + recv[s]
        out[...] = (gram * scale).astype(out.dtype)


def chip_sum_kernel(chips, *refs):
    recv, outs, total = refs[:chips], refs[chips:-1], refs[-1]
    acc = recv[-1][...]
    for ref in recv[:-1]:
        acc = acc + ref[...].astype(jnp.float32)
    total[...] = acc
    rows = outs[0].shape[0]
    me = lax.axis_index("z")
    for s, out in zip(slots(len(outs)), outs):
        base = pl.multiple_of(lax.bitwise_xor(me, s) * rows, rows)
        out[...] = total[pl.ds(base, rows), :]


def gram(recv, cells_one, plane, scale, tiled):
    deep = len(recv) // 2
    part, width = recv[0].shape
    steps = cells_one // plane
    ranks = part // steps
    block = width // plane
    rows = 2 * deep
    cells = rows * cells_one
    halves = plane // 4
    cells_out = cells // (2 * halves)
    swap = [(0, 1), (1, 0)]
    if not tiled:
        flat = jnp.stack(recv[:deep][::-1] + recv[deep:][::-1])
        flat = flat.reshape(2, deep, ranks, steps, plane, block)
        flat = jnp.take(flat, lax.axis_index("z") ^ jnp.arange(deep), axis=1)
        flat = jnp.take(flat, lax.axis_index("x") ^ jnp.arange(2), axis=0)
        flat = flat.transpose(1, 0, 4, 3, 2, 5).reshape(cells, ranks * block)
        whole = gram_block(flat, flat).reshape(rows, cells_one, halves, 2, cells_out)
        whole = whole.transpose(3, 0, 2, 1, 4).reshape(2, rows * halves, cells_one, cells_out)
        core = lax.axis_index("core")
        sent = lax.ppermute(jnp.take(whole, 1 - core, axis=0), "core", swap)
        parts = ((jnp.take(whole, core, axis=0) + sent) * scale).astype(jnp.bfloat16)
        parts = lax.all_to_all(
            parts, ("z", "x", "y"), split_axis=0, concat_axis=0, tiled=True
        )
        return jnp.sum(parts.astype(jnp.float32), axis=0)
    params = pltpu.CompilerParams(vmem_limit_bytes=20 * MIB)
    chips = 2 * halves
    flat = jax.ShapeDtypeStruct((cells, ranks * block), jnp.bfloat16)
    half = pl.pallas_call(
        functools.partial(first_side_kernel, plane),
        out_shape=flat,
        in_specs=in_vmem(deep),
        out_specs=in_vmem(1)[0],
        compiler_params=params,
        name="first_side",
    )(*recv[:deep])
    flat, other = pl.pallas_call(
        functools.partial(other_core_gram_kernel, plane),
        out_shape=[flat, jax.ShapeDtypeStruct((chips, cells // 2, cells_out), jnp.float32)],
        in_specs=in_vmem(deep + 1),
        out_specs=in_vmem(2),
        input_output_aliases={deep: 0},
        compiler_params=params,
        name="other_core_gram",
    )(*recv[deep:], half)
    other = lax.ppermute(other, "core", swap)
    sent = jax.ShapeDtypeStruct((cells // 2, cells_out), jnp.bfloat16)
    kept = jax.ShapeDtypeStruct((cells // 2, cells_out), jnp.float32)
    parts = pl.pallas_call(
        functools.partial(own_core_gram_kernel, scale),
        out_shape=[sent] * (chips - 1) + [kept],
        in_specs=in_vmem(2),
        out_specs=in_vmem(chips),
        compiler_params=params,
        name="own_core_gram",
    )(flat, other)
    parts = exchange(parts, ("x", "y"), slots(chips))
    parts = pl.pallas_call(
        functools.partial(chip_sum_kernel, chips),
        out_shape=[jax.ShapeDtypeStruct((cells_one, cells_out), jnp.float32)] * deep,
        in_specs=in_vmem(chips),
        out_specs=in_vmem(deep),
        scratch_shapes=[VMEM((cells // 2, cells_out), jnp.float32)],
        compiler_params=params,
        name="chip_sum",
    )(*parts)
    return sum(exchange(parts, "z", slots(deep)))


def exchange(pieces, axis, order):
    count = len(pieces)
    assert count & (count - 1) == 0
    return [
        lax.ppermute(piece, axis, [(i, i ^ s) for i in range(count)]) if s else piece
        for s, piece in zip(order, pieces)
    ]


def on_device(deep, cols, snapshot, basis_two, basis_three):
    cells_one = snapshot.shape[0]
    ranks_two, ranks_three = basis_two.shape[1], basis_three.shape[1]
    scale = 1.0 / (ranks_two * ranks_three)
    plane = 2 * cols
    steps = cells_one // plane
    tiled = (
        ranks_two == 128
        and ranks_three == 128
        and steps % 8 == 0
        and ranks_two // deep % plane == 0
        and 2 * deep * cells_one // cols % 128 == 0
    )
    pieces = project_three(snapshot, basis_two, basis_three, plane, cols, tiled)
    pieces = exchange(pieces, PLANE, plane_slots(plane))
    shares, factor = [], None
    for side in (pieces[:cols], pieces[cols:]):
        share, factor = project_two(side, factor, steps, deep, tiled)
        shares += exchange(share, "z", slots(deep))
    return gram(shares, cells_one, plane, scale, tiled)


def solution(mesh):
    rows, cols = mesh.shape["row"], mesh.shape["col"]
    devices = mesh.devices.reshape(rows // 2, 2, cols // 2, 2)
    row, col = ("z", "x"), ("y", "core")
    return jax.shard_map(
        functools.partial(on_device, rows // 2, cols),
        mesh=Mesh(devices, row + col),
        in_specs=(P(row, col, None), P(col, None), P()),
        out_specs=P(row, col),
        check_vma=False,
    )
```

```python
import functools

import jax
import jax.numpy as jnp
from jax import lax
from jax.experimental import pallas as pl
from jax.experimental.pallas import tpu as pltpu
from jax.sharding import Mesh
from jax.sharding import PartitionSpec as P

VMEM = pltpu.VMEM
MIB = 1024 * 1024
PLANE = ("x", "y", "core")


def in_vmem(count):
    return [pl.BlockSpec(memory_space=VMEM)] * count


def slots(count):
    return list(reversed(range(count)))


def plane_slots(plane):
    cols = plane // 2
    return [s ^ 1 for s in slots(cols)[: cols - 2]] + [1, 0] + list(range(cols, plane))


def place(axes):
    index = 0
    for axis in axes:
        index = index * lax.axis_size(axis) + lax.axis_index(axis)
    return index


def swap_blocks(tiles, width, me=None):
    tiles = list(tiles)
    lane = lax.broadcasted_iota(jnp.int32, tiles[0].shape, 1) // width
    lanes = len(tiles) * width
    step = 1
    while step < len(tiles):
        low = lax.bitwise_and(lane, step) == 0
        for i in range(len(tiles)):
            if i & step:
                continue
            one, two = tiles[i], tiles[i | step]
            zeros = jnp.where(low, one, pltpu.roll(two, step * width, 1))
            ones = jnp.where(low, pltpu.roll(one, lanes - step * width, 1), two)
            if me is None:
                tiles[i], tiles[i | step] = zeros, ones
            else:
                flip = lax.bitwise_and(me, step) != 0
                tiles[i] = jnp.where(flip, ones, zeros)
                tiles[i | step] = jnp.where(flip, zeros, ones)
        step *= 2
    return tiles


def bits(count):
    return [1 << bit for bit in range(count.bit_length() - 1)]


def flip_blocks(tile, width, step):
    lane = lax.broadcasted_iota(jnp.int32, tile.shape, 1) // width
    low = lax.bitwise_and(lane, step) == 0
    lanes = tile.shape[1]
    up = pltpu.roll(tile, step * width, 1)
    if 2 * step * width == lanes:
        return up
    return jnp.where(low, pltpu.roll(tile, lanes - step * width, 1), up)


def project_three_kernel(parts, snap, three, two, *rest):
    groups, steps, cells_two, cells_three = snap.shape
    outs = rest[:groups]
    buf, three_buf, two_buf, sems = rest[groups:]
    per = steps // parts
    rows = per * cells_two
    width = three.shape[1] // groups
    me = place(PLANE)
    copies = [
        pltpu.make_async_copy(three, three_buf.at[0], sems.at[parts]),
        pltpu.make_async_copy(two, two_buf, sems.at[parts + 1]),
    ]
    for n in range(parts):
        part = (slice(None), pl.ds(n * per, per))
        copies.append(pltpu.make_async_copy(snap.at[part], buf.at[part], sems.at[n]))
    for copy in copies:
        copy.start()
    copies[0].wait()
    for step in bits(groups):
        for g in range(step):
            tile = three_buf[g].astype(jnp.float32)
            three_buf[g | step] = flip_blocks(tile, width, step).astype(jnp.bfloat16)
    lane = lax.broadcasted_iota(jnp.int32, (rows, three.shape[1]), 1) // width
    keep = {step: lax.bitwise_and(lax.bitwise_xor(lane, me), step) == 0 for step in bits(groups)}
    for n in range(parts):
        copies[2 + n].wait()
        tiles = [
            jnp.dot(
                buf[g, n * per : (n + 1) * per].reshape(rows, cells_three),
                three_buf[g],
                preferred_element_type=jnp.float32,
            )
            for g in range(groups)
        ]
        for step in bits(groups):
            for i in range(groups):
                if i & step == 0:
                    one, two_tile = tiles[i], tiles[i | step]
                    tiles[i] = jnp.where(keep[step], one, two_tile)
                    tiles[i | step] = jnp.where(keep[step], two_tile, one)
        for s, out in zip(plane_slots(groups), outs):
            out[n * rows : (n + 1) * rows, :] = tiles[s].astype(jnp.bfloat16)
    copies[1].wait()
    for out in outs:
        if out.shape[0] > steps * cells_two:
            out[steps * cells_two :, :] = two_buf[...]


def project_three(snapshot, basis_two, basis_three, plane, cols, tiled):
    cells_one, cells_two, cells_three = snapshot.shape
    ranks_three = basis_three.shape[1]
    steps = cells_one // plane
    snap = snapshot.reshape(plane, steps, cells_two, cells_three)
    if not tiled:
        inner = jnp.einsum(
            "gtbc,cr->gtbr", snap, basis_three, preferred_element_type=jnp.float32
        ).astype(jnp.bfloat16)
        inner = inner.reshape(plane, steps, cells_two, plane, ranks_three // plane)
        inner = inner.transpose(3, 1, 2, 0, 4)
        inner = inner.reshape(plane, steps * cells_two, ranks_three)
        pieces = [jnp.take(inner, place(PLANE) ^ s, axis=0) for s in plane_slots(plane)]
        return [
            jnp.concatenate([piece, basis_two]) if s < cols else piece
            for s, piece in zip(plane_slots(plane), pieces)
        ]
    parts = 2
    outs = [
        jax.ShapeDtypeStruct(((steps + (s < cols)) * cells_two, ranks_three), jnp.bfloat16)
        for s in plane_slots(plane)
    ]
    args = [
        pltpu.with_memory_space_constraint(arg, pltpu.HBM)
        for arg in (snap, basis_three, basis_two)
    ]
    return pl.pallas_call(
        functools.partial(project_three_kernel, parts),
        out_shape=outs,
        in_specs=[pl.BlockSpec(memory_space=pltpu.HBM)] * 3,
        out_specs=in_vmem(plane),
        scratch_shapes=[
            VMEM(snap.shape, jnp.bfloat16),
            VMEM((plane,) + basis_three.shape, jnp.bfloat16),
            VMEM(basis_two.shape, jnp.bfloat16),
            pltpu.SemaphoreType.DMA((parts + 2,)),
        ],
        compiler_params=pltpu.CompilerParams(vmem_limit_bytes=20 * MIB),
        name="project_three",
    )(*args)


def project_two_kernel(cols, steps, first, *refs):
    recv = refs[:cols]
    if first:
        outs, factor_ref, held = refs[cols:-2], refs[-2], refs[-1]
        cells = recv[0].shape[0] // (steps + 1)
        factor = jnp.concatenate([ref[steps * cells :, :] for ref in recv], axis=0)
        factor = factor.astype(jnp.float32).T.astype(jnp.bfloat16)
        factor_ref[...] = factor
    else:
        recv = [*[recv[i ^ 1] for i in range(cols - 1, 1, -1)], recv[1], recv[0]]
        factor, outs, held = refs[cols][...], refs[cols + 1 : -1], refs[-1]
        cells = recv[0].shape[0] // steps
    part, ranks_two = outs[0].shape
    me = lax.axis_index("z")
    for t in range(steps):
        inner = jnp.concatenate(
            [ref[t * cells : (t + 1) * cells, :] for ref in recv], axis=0
        )
        held[pl.ds(t, ranks_two, stride=steps), :] = jnp.dot(
            factor, inner, preferred_element_type=jnp.float32
        )
    for s, out in zip(slots(len(outs)), outs):
        base = pl.multiple_of(lax.bitwise_xor(me, s) * part, part)
        out[...] = held[pl.ds(base, part), :].astype(jnp.bfloat16)


def project_two(recv, factor, steps, deep, tiled):
    cols = len(recv)
    first = factor is None
    height, width = recv[0].shape
    cells_two = height // (steps + first)
    part = steps * width // deep
    if not tiled:
        if not first:
            recv = [*[recv[i ^ 1] for i in range(cols - 1, 1, -1)], recv[1], recv[0]]
        else:
            factor = jnp.concatenate([piece[steps * cells_two :] for piece in recv]).T
        inner = jnp.stack([piece[: steps * cells_two] for piece in recv])
        inner = inner.reshape(cols, steps, cells_two, width)
        full = jnp.einsum(
            "jtbl,qjb->qtl",
            inner,
            factor.reshape(width, cols, cells_two),
            preferred_element_type=jnp.float32,
        )
        full = full.astype(jnp.bfloat16).reshape(deep, part, width)
        return [jnp.take(full, lax.axis_index("z") ^ s, axis=0) for s in slots(deep)], factor
    outs = [jax.ShapeDtypeStruct((part, width), jnp.bfloat16)] * deep
    if first:
        outs.append(jax.ShapeDtypeStruct((width, cols * cells_two), jnp.bfloat16))
    args = recv if first else recv + [factor]
    outs = pl.pallas_call(
        functools.partial(project_two_kernel, cols, steps, first),
        out_shape=outs,
        in_specs=in_vmem(len(args)),
        out_specs=in_vmem(len(outs)),
        scratch_shapes=[VMEM((steps * width, width), jnp.float32)],
        compiler_params=pltpu.CompilerParams(vmem_limit_bytes=20 * MIB),
        name="project_two",
    )(*args)
    return (outs[:deep], outs[deep]) if first else (outs, factor)


def gram_block(left, right):
    return lax.dot_general(
        left, right, (((1,), (1,)), ((), ())), preferred_element_type=jnp.float32
    )


def fill_side(plane, side, recv, flat):
    deep = len(recv)
    cells_one = flat.shape[0] // (2 * deep)
    part, width = recv[0].shape
    steps = cells_one // plane
    me_z, me_x = lax.axis_index("z"), lax.axis_index("x")
    for s, ref in zip(slots(deep), recv):
        row = lax.bitwise_xor(me_z, s) * 2 + lax.bitwise_xor(me_x, side)
        base = pl.multiple_of(row * cells_one, cells_one)
        for u in range(part // steps // plane):
            tiles = ref[u * plane * steps : (u + 1) * plane * steps, :].astype(jnp.float32)
            tiles = [tiles[q * steps : (q + 1) * steps] for q in range(plane)]
            stacked = jnp.concatenate(swap_blocks(tiles, width // plane, place(PLANE)), axis=0)
            flat[pl.ds(base, cells_one), u * width : (u + 1) * width] = stacked.astype(
                jnp.bfloat16
            )


def first_side_kernel(plane, *refs):
    fill_side(plane, 0, refs[:-1], refs[-1])


def chip_block(flat, slot, core, cells_out):
    halves = lax.axis_size("y")
    deep = lax.axis_size("z")
    cells_one = flat.shape[0] // (2 * deep)
    where = lax.bitwise_xor(place(("x", "y")), slot)
    x, y = where // halves, lax.rem(where, halves)
    left = [
        flat[pl.ds(pl.multiple_of((2 * z + x) * cells_one, cells_one), cells_one), :]
        for z in range(deep)
    ]
    base = pl.multiple_of((2 * y + core) * cells_out, cells_out)
    return gram_block(jnp.concatenate(left, axis=0), flat[pl.ds(base, cells_out), :])


def other_core_gram_kernel(plane, *refs):
    recv, (half, flat, out) = refs[:-3], refs[-3:]
    fill_side(plane, 1, recv, flat)
    core = 1 - lax.axis_index("core")
    for s in range(out.shape[0]):
        out[s] = chip_block(flat, s, core, out.shape[2])


def own_core_gram_kernel(scale, flat, recv, *outs):
    core = lax.axis_index("core")
    for s, out in zip(slots(len(outs)), outs):
        gram = chip_block(flat, s, core, out.shape[1]) + recv[s]
        out[...] = (gram * scale).astype(out.dtype)


def chip_sum_kernel(chips, *refs):
    recv, outs, total = refs[:chips], refs[chips:-1], refs[-1]
    acc = recv[-1][...]
    for ref in recv[:-1]:
        acc = acc + ref[...].astype(jnp.float32)
    total[...] = acc
    rows = outs[0].shape[0]
    me = lax.axis_index("z")
    for s, out in zip(slots(len(outs)), outs):
        base = pl.multiple_of(lax.bitwise_xor(me, s) * rows, rows)
        out[...] = total[pl.ds(base, rows), :]


def gram(recv, cells_one, plane, scale, tiled):
    deep = len(recv) // 2
    part, width = recv[0].shape
    steps = cells_one // plane
    ranks = part // steps
    block = width // plane
    rows = 2 * deep
    cells = rows * cells_one
    halves = plane // 4
    cells_out = cells // (2 * halves)
    swap = [(0, 1), (1, 0)]
    if not tiled:
        flat = jnp.stack(recv[:deep][::-1] + recv[deep:][::-1])
        flat = flat.reshape(2, deep, ranks, steps, plane, block)
        flat = jnp.take(flat, lax.axis_index("z") ^ jnp.arange(deep), axis=1)
        flat = jnp.take(flat, lax.axis_index("x") ^ jnp.arange(2), axis=0)
        flat = flat.transpose(1, 0, 4, 3, 2, 5).reshape(cells, ranks * block)
        whole = gram_block(flat, flat).reshape(rows, cells_one, halves, 2, cells_out)
        whole = whole.transpose(3, 0, 2, 1, 4).reshape(2, rows * halves, cells_one, cells_out)
        core = lax.axis_index("core")
        sent = lax.ppermute(jnp.take(whole, 1 - core, axis=0), "core", swap)
        parts = ((jnp.take(whole, core, axis=0) + sent) * scale).astype(jnp.bfloat16)
        parts = lax.all_to_all(
            parts, ("z", "x", "y"), split_axis=0, concat_axis=0, tiled=True
        )
        return jnp.sum(parts.astype(jnp.float32), axis=0)
    params = pltpu.CompilerParams(vmem_limit_bytes=20 * MIB)
    chips = 2 * halves
    flat = jax.ShapeDtypeStruct((cells, ranks * block), jnp.bfloat16)
    half = pl.pallas_call(
        functools.partial(first_side_kernel, plane),
        out_shape=flat,
        in_specs=in_vmem(deep),
        out_specs=in_vmem(1)[0],
        compiler_params=params,
        name="first_side",
    )(*recv[:deep])
    flat, other = pl.pallas_call(
        functools.partial(other_core_gram_kernel, plane),
        out_shape=[flat, jax.ShapeDtypeStruct((chips, cells // 2, cells_out), jnp.float32)],
        in_specs=in_vmem(deep + 1),
        out_specs=in_vmem(2),
        input_output_aliases={deep: 0},
        compiler_params=params,
        name="other_core_gram",
    )(*recv[deep:], half)
    other = lax.ppermute(other, "core", swap)
    sent = jax.ShapeDtypeStruct((cells // 2, cells_out), jnp.bfloat16)
    kept = jax.ShapeDtypeStruct((cells // 2, cells_out), jnp.float32)
    parts = pl.pallas_call(
        functools.partial(own_core_gram_kernel, scale),
        out_shape=[sent] * (chips - 1) + [kept],
        in_specs=in_vmem(2),
        out_specs=in_vmem(chips),
        compiler_params=params,
        name="own_core_gram",
    )(flat, other)
    parts = exchange(parts, ("x", "y"), slots(chips))
    parts = pl.pallas_call(
        functools.partial(chip_sum_kernel, chips),
        out_shape=[jax.ShapeDtypeStruct((cells_one, cells_out), jnp.float32)] * deep,
        in_specs=in_vmem(chips),
        out_specs=in_vmem(deep),
        scratch_shapes=[VMEM((cells // 2, cells_out), jnp.float32)],
        compiler_params=params,
        name="chip_sum",
    )(*parts)
    return sum(exchange(parts, "z", slots(deep)))


def exchange(pieces, axis, order):
    count = len(pieces)
    assert count & (count - 1) == 0
    return [
        lax.ppermute(piece, axis, [(i, i ^ s) for i in range(count)]) if s else piece
        for s, piece in zip(order, pieces)
    ]


def on_device(deep, cols, snapshot, basis_two, basis_three):
    cells_one = snapshot.shape[0]
    ranks_two, ranks_three = basis_two.shape[1], basis_three.shape[1]
    scale = 1.0 / (ranks_two * ranks_three)
    plane = 2 * cols
    steps = cells_one // plane
    tiled = (
        ranks_two == 128
        and ranks_three == 128
        and steps % 8 == 0
        and ranks_two // deep % plane == 0
        and 2 * deep * cells_one // cols % 128 == 0
    )
    pieces = project_three(snapshot, basis_two, basis_three, plane, cols, tiled)
    pieces = exchange(pieces, PLANE, plane_slots(plane))
    shares, factor = [], None
    for side in (pieces[:cols], pieces[cols:]):
        share, factor = project_two(side, factor, steps, deep, tiled)
        shares += exchange(share, "z", slots(deep))
    return gram(shares, cells_one, plane, scale, tiled)


def solution(mesh):
    rows, cols = mesh.shape["row"], mesh.shape["col"]
    devices = mesh.devices.reshape(rows // 2, 2, cols // 2, 2)
    row, col = ("z", "x"), ("y", "core")
    return jax.shard_map(
        functools.partial(on_device, rows // 2, cols),
        mesh=Mesh(devices, row + col),
        in_specs=(P(row, col, None), P(col, None), P()),
        out_specs=P(row, col),
        check_vma=False,
    )
```

```python
import functools

import jax
import jax.numpy as jnp
from jax import lax
from jax.experimental import pallas as pl
from jax.experimental.pallas import tpu as pltpu
from jax.sharding import Mesh
from jax.sharding import PartitionSpec as P

VMEM = pltpu.VMEM
MIB = 1024 * 1024
PLANE = ("x", "y", "core")


def in_vmem(count):
    return [pl.BlockSpec(memory_space=VMEM)] * count


def slots(count):
    return list(reversed(range(count)))


def plane_slots(plane):
    cols = plane // 2
    return [s ^ 1 for s in slots(cols)[: cols - 2]] + [1, 0] + list(range(cols, plane))


def place(axes):
    index = 0
    for axis in axes:
        index = index * lax.axis_size(axis) + lax.axis_index(axis)
    return index


def swap_blocks(tiles, width, me=None):
    tiles = list(tiles)
    lane = lax.broadcasted_iota(jnp.int32, tiles[0].shape, 1) // width
    lanes = len(tiles) * width
    step = 1
    while step < len(tiles):
        low = lax.bitwise_and(lane, step) == 0
        for i in range(len(tiles)):
            if i & step:
                continue
            one, two = tiles[i], tiles[i | step]
            zeros = jnp.where(low, one, pltpu.roll(two, step * width, 1))
            ones = jnp.where(low, pltpu.roll(one, lanes - step * width, 1), two)
            if me is None:
                tiles[i], tiles[i | step] = zeros, ones
            else:
                flip = lax.bitwise_and(me, step) != 0
                tiles[i] = jnp.where(flip, ones, zeros)
                tiles[i | step] = jnp.where(flip, zeros, ones)
        step *= 2
    return tiles


def bits(count):
    return [1 << bit for bit in range(count.bit_length() - 1)]


def flip_blocks(tile, width, step):
    lane = lax.broadcasted_iota(jnp.int32, tile.shape, 1) // width
    low = lax.bitwise_and(lane, step) == 0
    lanes = tile.shape[1]
    up = pltpu.roll(tile, step * width, 1)
    if 2 * step * width == lanes:
        return up
    return jnp.where(low, pltpu.roll(tile, lanes - step * width, 1), up)


def project_three_kernel(parts, snap, three, two, *rest):
    groups, steps, cells_two, cells_three = snap.shape
    outs = rest[:groups]
    buf, three_buf, two_buf, sems = rest[groups:]
    per = steps // parts
    rows = per * cells_two
    width = three.shape[1] // groups
    me = place(PLANE)
    copies = [
        pltpu.make_async_copy(three, three_buf.at[0], sems.at[parts]),
        pltpu.make_async_copy(two, two_buf, sems.at[parts + 1]),
    ]
    for n in range(parts):
        part = (slice(None), pl.ds(n * per, per))
        copies.append(pltpu.make_async_copy(snap.at[part], buf.at[part], sems.at[n]))
    for copy in copies:
        copy.start()
    copies[0].wait()
    for step in bits(groups):
        for g in range(step):
            tile = three_buf[g].astype(jnp.float32)
            three_buf[g | step] = flip_blocks(tile, width, step).astype(jnp.bfloat16)
    lane = lax.broadcasted_iota(jnp.int32, (rows, three.shape[1]), 1) // width
    keep = {step: lax.bitwise_and(lax.bitwise_xor(lane, me), step) == 0 for step in bits(groups)}
    for n in range(parts):
        copies[2 + n].wait()
        tiles = [
            jnp.dot(
                buf[g, n * per : (n + 1) * per].reshape(rows, cells_three),
                three_buf[g],
                preferred_element_type=jnp.float32,
            )
            for g in range(groups)
        ]
        for step in bits(groups):
            for i in range(groups):
                if i & step == 0:
                    one, two_tile = tiles[i], tiles[i | step]
                    tiles[i] = jnp.where(keep[step], one, two_tile)
                    tiles[i | step] = jnp.where(keep[step], two_tile, one)
        for s, out in zip(plane_slots(groups), outs):
            out[n * rows : (n + 1) * rows, :] = tiles[s].astype(jnp.bfloat16)
    copies[1].wait()
    for out in outs:
        if out.shape[0] > steps * cells_two:
            out[steps * cells_two :, :] = two_buf[...]


def project_three(snapshot, basis_two, basis_three, plane, cols, tiled):
    cells_one, cells_two, cells_three = snapshot.shape
    ranks_three = basis_three.shape[1]
    steps = cells_one // plane
    snap = snapshot.reshape(plane, steps, cells_two, cells_three)
    if not tiled:
        inner = jnp.einsum(
            "gtbc,cr->gtbr", snap, basis_three, preferred_element_type=jnp.float32
        ).astype(jnp.bfloat16)
        inner = inner.reshape(plane, steps, cells_two, plane, ranks_three // plane)
        inner = inner.transpose(3, 1, 2, 0, 4)
        inner = inner.reshape(plane, steps * cells_two, ranks_three)
        pieces = [jnp.take(inner, place(PLANE) ^ s, axis=0) for s in plane_slots(plane)]
        return [
            jnp.concatenate([piece, basis_two]) if s < cols else piece
            for s, piece in zip(plane_slots(plane), pieces)
        ]
    parts = 4
    outs = [
        jax.ShapeDtypeStruct(((steps + (s < cols)) * cells_two, ranks_three), jnp.bfloat16)
        for s in plane_slots(plane)
    ]
    args = [
        pltpu.with_memory_space_constraint(arg, pltpu.HBM)
        for arg in (snap, basis_three, basis_two)
    ]
    return pl.pallas_call(
        functools.partial(project_three_kernel, parts),
        out_shape=outs,
        in_specs=[pl.BlockSpec(memory_space=pltpu.HBM)] * 3,
        out_specs=in_vmem(plane),
        scratch_shapes=[
            VMEM(snap.shape, jnp.bfloat16),
            VMEM((plane,) + basis_three.shape, jnp.bfloat16),
            VMEM(basis_two.shape, jnp.bfloat16),
            pltpu.SemaphoreType.DMA((parts + 2,)),
        ],
        compiler_params=pltpu.CompilerParams(vmem_limit_bytes=20 * MIB),
        name="project_three",
    )(*args)


def project_two_kernel(cols, steps, first, *refs):
    recv = refs[:cols]
    if first:
        outs, factor_ref, held = refs[cols:-2], refs[-2], refs[-1]
        cells = recv[0].shape[0] // (steps + 1)
        factor = jnp.concatenate([ref[steps * cells :, :] for ref in recv], axis=0)
        factor = factor.astype(jnp.float32).T.astype(jnp.bfloat16)
        factor_ref[...] = factor
    else:
        recv = [*[recv[i ^ 1] for i in range(cols - 1, 1, -1)], recv[1], recv[0]]
        factor, outs, held = refs[cols][...], refs[cols + 1 : -1], refs[-1]
        cells = recv[0].shape[0] // steps
    part, ranks_two = outs[0].shape
    me = lax.axis_index("z")
    for t in range(steps):
        inner = jnp.concatenate(
            [ref[t * cells : (t + 1) * cells, :] for ref in recv], axis=0
        )
        held[pl.ds(t, ranks_two, stride=steps), :] = jnp.dot(
            factor, inner, preferred_element_type=jnp.float32
        )
    for s, out in zip(slots(len(outs)), outs):
        base = pl.multiple_of(lax.bitwise_xor(me, s) * part, part)
        out[...] = held[pl.ds(base, part), :].astype(jnp.bfloat16)


def project_two(recv, factor, steps, deep, tiled):
    cols = len(recv)
    first = factor is None
    height, width = recv[0].shape
    cells_two = height // (steps + first)
    part = steps * width // deep
    if not tiled:
        if not first:
            recv = [*[recv[i ^ 1] for i in range(cols - 1, 1, -1)], recv[1], recv[0]]
        else:
            factor = jnp.concatenate([piece[steps * cells_two :] for piece in recv]).T
        inner = jnp.stack([piece[: steps * cells_two] for piece in recv])
        inner = inner.reshape(cols, steps, cells_two, width)
        full = jnp.einsum(
            "jtbl,qjb->qtl",
            inner,
            factor.reshape(width, cols, cells_two),
            preferred_element_type=jnp.float32,
        )
        full = full.astype(jnp.bfloat16).reshape(deep, part, width)
        return [jnp.take(full, lax.axis_index("z") ^ s, axis=0) for s in slots(deep)], factor
    outs = [jax.ShapeDtypeStruct((part, width), jnp.bfloat16)] * deep
    if first:
        outs.append(jax.ShapeDtypeStruct((width, cols * cells_two), jnp.bfloat16))
    args = recv if first else recv + [factor]
    outs = pl.pallas_call(
        functools.partial(project_two_kernel, cols, steps, first),
        out_shape=outs,
        in_specs=in_vmem(len(args)),
        out_specs=in_vmem(len(outs)),
        scratch_shapes=[VMEM((steps * width, width), jnp.float32)],
        compiler_params=pltpu.CompilerParams(vmem_limit_bytes=20 * MIB),
        name="project_two",
    )(*args)
    return (outs[:deep], outs[deep]) if first else (outs, factor)


def gram_block(left, right):
    return lax.dot_general(
        left, right, (((1,), (1,)), ((), ())), preferred_element_type=jnp.float32
    )


def fill_side(plane, side, recv, flat):
    deep = len(recv)
    cells_one = flat.shape[0] // (2 * deep)
    part, width = recv[0].shape
    steps = cells_one // plane
    me_z, me_x = lax.axis_index("z"), lax.axis_index("x")
    for s, ref in zip(slots(deep), recv):
        row = lax.bitwise_xor(me_z, s) * 2 + lax.bitwise_xor(me_x, side)
        base = pl.multiple_of(row * cells_one, cells_one)
        for u in range(part // steps // plane):
            tiles = ref[u * plane * steps : (u + 1) * plane * steps, :].astype(jnp.float32)
            tiles = [tiles[q * steps : (q + 1) * steps] for q in range(plane)]
            stacked = jnp.concatenate(swap_blocks(tiles, width // plane, place(PLANE)), axis=0)
            flat[pl.ds(base, cells_one), u * width : (u + 1) * width] = stacked.astype(
                jnp.bfloat16
            )


def first_side_kernel(plane, *refs):
    fill_side(plane, 0, refs[:-1], refs[-1])


def chip_block(flat, slot, core, cells_out):
    halves = lax.axis_size("y")
    deep = lax.axis_size("z")
    cells_one = flat.shape[0] // (2 * deep)
    where = lax.bitwise_xor(place(("x", "y")), slot)
    x, y = where // halves, lax.rem(where, halves)
    left = [
        flat[pl.ds(pl.multiple_of((2 * z + x) * cells_one, cells_one), cells_one), :]
        for z in range(deep)
    ]
    base = pl.multiple_of((2 * y + core) * cells_out, cells_out)
    return gram_block(jnp.concatenate(left, axis=0), flat[pl.ds(base, cells_out), :])


def other_core_gram_kernel(plane, *refs):
    recv, (half, flat, out) = refs[:-3], refs[-3:]
    fill_side(plane, 1, recv, flat)
    core = 1 - lax.axis_index("core")
    for s in range(out.shape[0]):
        out[s] = chip_block(flat, s, core, out.shape[2])


def own_core_gram_kernel(scale, flat, recv, *outs):
    core = lax.axis_index("core")
    for s, out in zip(slots(len(outs)), outs):
        gram = chip_block(flat, s, core, out.shape[1]) + recv[s]
        out[...] = (gram * scale).astype(out.dtype)


def chip_sum_kernel(chips, *refs):
    recv, outs, total = refs[:chips], refs[chips:-1], refs[-1]
    acc = recv[-1][...]
    for ref in recv[:-1]:
        acc = acc + ref[...].astype(jnp.float32)
    total[...] = acc
    rows = outs[0].shape[0]
    me = lax.axis_index("z")
    for s, out in zip(slots(len(outs)), outs):
        base = pl.multiple_of(lax.bitwise_xor(me, s) * rows, rows)
        out[...] = total[pl.ds(base, rows), :]


def gram(recv, cells_one, plane, scale, tiled):
    deep = len(recv) // 2
    part, width = recv[0].shape
    steps = cells_one // plane
    ranks = part // steps
    block = width // plane
    rows = 2 * deep
    cells = rows * cells_one
    halves = plane // 4
    cells_out = cells // (2 * halves)
    swap = [(0, 1), (1, 0)]
    if not tiled:
        flat = jnp.stack(recv[:deep][::-1] + recv[deep:][::-1])
        flat = flat.reshape(2, deep, ranks, steps, plane, block)
        flat = jnp.take(flat, lax.axis_index("z") ^ jnp.arange(deep), axis=1)
        flat = jnp.take(flat, lax.axis_index("x") ^ jnp.arange(2), axis=0)
        flat = flat.transpose(1, 0, 4, 3, 2, 5).reshape(cells, ranks * block)
        whole = gram_block(flat, flat).reshape(rows, cells_one, halves, 2, cells_out)
        whole = whole.transpose(3, 0, 2, 1, 4).reshape(2, rows * halves, cells_one, cells_out)
        core = lax.axis_index("core")
        sent = lax.ppermute(jnp.take(whole, 1 - core, axis=0), "core", swap)
        parts = ((jnp.take(whole, core, axis=0) + sent) * scale).astype(jnp.bfloat16)
        parts = lax.all_to_all(
            parts, ("z", "x", "y"), split_axis=0, concat_axis=0, tiled=True
        )
        return jnp.sum(parts.astype(jnp.float32), axis=0)
    params = pltpu.CompilerParams(vmem_limit_bytes=20 * MIB)
    chips = 2 * halves
    flat = jax.ShapeDtypeStruct((cells, ranks * block), jnp.bfloat16)
    half = pl.pallas_call(
        functools.partial(first_side_kernel, plane),
        out_shape=flat,
        in_specs=in_vmem(deep),
        out_specs=in_vmem(1)[0],
        compiler_params=params,
        name="first_side",
    )(*recv[:deep])
    flat, other = pl.pallas_call(
        functools.partial(other_core_gram_kernel, plane),
        out_shape=[flat, jax.ShapeDtypeStruct((chips, cells // 2, cells_out), jnp.float32)],
        in_specs=in_vmem(deep + 1),
        out_specs=in_vmem(2),
        input_output_aliases={deep: 0},
        compiler_params=params,
        name="other_core_gram",
    )(*recv[deep:], half)
    other = lax.ppermute(other, "core", swap)
    sent = jax.ShapeDtypeStruct((cells // 2, cells_out), jnp.bfloat16)
    kept = jax.ShapeDtypeStruct((cells // 2, cells_out), jnp.float32)
    parts = pl.pallas_call(
        functools.partial(own_core_gram_kernel, scale),
        out_shape=[sent] * (chips - 1) + [kept],
        in_specs=in_vmem(2),
        out_specs=in_vmem(chips),
        compiler_params=params,
        name="own_core_gram",
    )(flat, other)
    parts = exchange(parts, ("x", "y"), slots(chips))
    parts = pl.pallas_call(
        functools.partial(chip_sum_kernel, chips),
        out_shape=[jax.ShapeDtypeStruct((cells_one, cells_out), jnp.float32)] * deep,
        in_specs=in_vmem(chips),
        out_specs=in_vmem(deep),
        scratch_shapes=[VMEM((cells // 2, cells_out), jnp.float32)],
        compiler_params=params,
        name="chip_sum",
    )(*parts)
    return sum(exchange(parts, "z", slots(deep)))


def exchange(pieces, axis, order):
    count = len(pieces)
    assert count & (count - 1) == 0
    return [
        lax.ppermute(piece, axis, [(i, i ^ s) for i in range(count)]) if s else piece
        for s, piece in zip(order, pieces)
    ]


def on_device(deep, cols, snapshot, basis_two, basis_three):
    cells_one = snapshot.shape[0]
    ranks_two, ranks_three = basis_two.shape[1], basis_three.shape[1]
    scale = 1.0 / (ranks_two * ranks_three)
    plane = 2 * cols
    steps = cells_one // plane
    tiled = (
        ranks_two == 128
        and ranks_three == 128
        and steps % 8 == 0
        and ranks_two // deep % plane == 0
        and 2 * deep * cells_one // cols % 128 == 0
    )
    pieces = project_three(snapshot, basis_two, basis_three, plane, cols, tiled)
    pieces = exchange(pieces, PLANE, plane_slots(plane))
    shares, factor = [], None
    for side in (pieces[:cols], pieces[cols:]):
        share, factor = project_two(side, factor, steps, deep, tiled)
        shares += exchange(share, "z", slots(deep))
    return gram(shares, cells_one, plane, scale, tiled)


def solution(mesh):
    rows, cols = mesh.shape["row"], mesh.shape["col"]
    devices = mesh.devices.reshape(rows // 2, 2, cols // 2, 2)
    row, col = ("z", "x"), ("y", "core")
    return jax.shard_map(
        functools.partial(on_device, rows // 2, cols),
        mesh=Mesh(devices, row + col),
        in_specs=(P(row, col, None), P(col, None), P()),
        out_specs=P(row, col),
        check_vma=False,
    )
```
